32 devices in a mesh: node: 8 (over z, x), freq: 4 (over y, core).
Axes of the slice: x: 2, y: 2, z: 4, core: 2. Of those that a mesh axis runs over, the one named last changes fastest.
Arguments:
- action_old: float32 [36, 36, 4096], P('freq', None, 'node'), may hold values from 0.05 to 2
- source: float32 [36, 36, 4096], P('freq', None, 'node'), may hold values from -4 to 4
- time_weight: float32 [4096], P('node'), may hold values from 0.5 to 4
- group_speed: float32 [36], P('freq'), may hold values from 0.3 to 3
- normals: float32 [2, 8, 4096], P(None, None, 'node'), may hold values from -3 to 3
- refract: float32 [4096], P('node'), may hold values from -4 to 4
- freq_shift: float32 [4096], P('node'), may hold values from -4 to 4
- nbr_list: int32 [8, 6], P('node'), may hold values from -1 to 7, as said below
- send_nodes: int32 [8, 6, 32], P('node'), may hold values from 0 to 511, as said below
- adjacency: int32 [8, 4096], P(None, 'node'), may hold values from 0 to 703, as said below
Outputs:
- action_new: float32 [36, 36, 4096], P('freq', None, 'node')
The draws below stay inside these ranges and needn't reach their ends.
Inputs may be any that keep to these rules, and one draw needn't show every extreme that they name: `nbr_list`: slot entries of subdomain p are distinct subdomains (p + o) or (p - o) modulo the number of subdomains, 1 <= o <= 3, or -1 for an empty slot; p + 1 and p - 1 are always listed; if p lists q then q lists p. `send_nodes`: local node indices of the sending subdomain. `adjacency`: entries as in the first step; an entry at or above 512 never names an empty slot.
All inputs are finite; a program needn't handle non-finite values.
Results may differ from the reference program's by a relative error of at most 0.000088.
Values sent between devices are 32-bit elements; how exact they have to be, the bound alone decides.
No kernel may reach another device: no remote copies, remote signals or barrier semaphores. Data moves between devices by JAX's collectives and lax.ppermute only.
A program may use at most 128 MiB of HBM per device.

```python
import math
import jax
import jax.numpy as jnp

FREQ = 36
DIR = 36
ND = 512
DEG = 8
REACH = 3
ITERS = 3
NB = 6
H = 32
NODES = 4096
N_NODE = 8


def neighbour_table(key):
    base = jax.random.fold_in(key, 11)
    subdomain = jnp.arange(N_NODE)
    columns = []
    for reach in range(1, REACH + 1):
        if reach == 1:
            linked = jnp.ones((N_NODE,), jnp.int32)
        else:
            linked = jax.random.randint(jax.random.fold_in(base, reach), (N_NODE,), 0, 2)
        upward = jnp.where(linked > 0, (subdomain + reach) % N_NODE, -1)
        downward = jnp.where(jnp.roll(linked, reach) > 0, (subdomain - reach) % N_NODE, -1)
        columns.append(upward)
        columns.append(downward)
    candidates = jnp.stack(columns, axis=1)
    scores = jax.random.randint(jax.random.fold_in(base, 99), (N_NODE, NB), 0, 1 << 16) * NB + jnp.arange(NB)[None, :]
    order = jnp.argsort(scores, axis=1)
    return jnp.take_along_axis(candidates, order, axis=1).astype(jnp.int32)


def draw_nbr_list(key, part):
    return neighbour_table(key)


def draw_send_nodes(key, part):
    return jax.random.randint(jax.random.fold_in(key, 5), (N_NODE, NB, H), 0, ND).astype(jnp.int32)


def draw_adjacency(key, part):
    table = neighbour_table(key)
    degree = jax.random.randint(jax.random.fold_in(key, 21), (N_NODE, ND), 3, DEG + 1)
    own_index = jnp.arange(ND)
    nearby = (own_index[None, None, :] + jax.random.randint(jax.random.fold_in(key, 22), (DEG, N_NODE, ND), 1, ND)) % ND
    halo_pos = jax.random.randint(jax.random.fold_in(key, 23), (DEG, N_NODE, ND), 0, NB * H)
    slot_live = jnp.repeat(table >= 0, H, axis=1)
    halo_live = jnp.take_along_axis(jnp.broadcast_to(slot_live[None], (DEG, N_NODE, NB * H)), halo_pos, axis=2)
    use_halo = (jax.random.randint(jax.random.fold_in(key, 24), (DEG, N_NODE, ND), 0, 100) < 15) & halo_live
    entry = jnp.where(use_halo, ND + halo_pos, nearby)
    scores = jax.random.randint(jax.random.fold_in(key, 25), (N_NODE, ND), 0, 1 << 16) * ND + own_index[None, :]
    ranking = jnp.argsort(jnp.argsort(scores, axis=1), axis=1)
    covered = ranking < NB * H
    cover_pos = jnp.where(covered, ranking, 0)
    cover_live = covered & jnp.take_along_axis(slot_live, cover_pos, axis=1)
    first = jnp.where(cover_live, ND + cover_pos, entry[0])
    entry = entry.at[0].set(first)
    levels = jnp.arange(DEG)[:, None, None]
    entry = jnp.where(levels < degree[None], entry, own_index[None, None, :])
    return entry.reshape(DEG, N_NODE * ND).astype(jnp.int32)


def steps_of(stream_key, shape, split, smallest, high):
    def one(dim, parts):
        draws = jax.random.uniform(jax.random.fold_in(jax.random.fold_in(stream_key, 6), dim), (parts,), jnp.float32, smallest / len(split), high / len(split))
        return jnp.repeat(jnp.exp(draws), shape[dim] // parts).reshape((-1,) + (1,) * (len(shape) - dim - 1))

    factor_of = one(*split[0])
    for cut in split[1:]:
        factor_of = factor_of * one(*cut)
    return factor_of


def scatter_about(own_key, extent, deviation, bound, cuts=(), held_as=jnp.bfloat16):
    result = deviation * jax.random.normal(own_key, extent, jnp.float32)
    if cuts:
        result = result * steps_of(own_key, extent, cuts, -0.22, 0.18)
    return jnp.clip(result, -bound, bound).astype(held_as)


def setup_inputs(seed: int = 0) -> dict:
    splits = jax.random.split(jax.random.key(seed), 11)
    action_old = jnp.clip(jnp.exp(math.log(2.0) - 3.6888794 * jax.random.uniform(splits[0], (FREQ, DIR, NODES), jnp.float32) ** steps_of(splits[0], (FREQ, DIR, NODES), ((0, 4), (2, 8)), -0.2, 0.2)), 0.05, 2.0)
    source = scatter_about(splits[1], (FREQ, DIR, NODES), 0.3, 4.0, ((0, 4), (2, 8)), jnp.float32)
    time_weight = jnp.clip(jnp.exp(math.log(4.0) - 2.0794415 * jax.random.uniform(splits[2], (NODES,), jnp.float32) ** steps_of(splits[2], (NODES,), ((0, 8),), -0.2, 0.2)), 0.5, 4.0)
    group_speed = jnp.clip(jnp.exp(math.log(3.0) - 2.3025851 * jax.random.uniform(splits[3], (FREQ,), jnp.float32) ** steps_of(splits[3], (FREQ,), ((0, 4),), -0.2, 0.2)), 0.3, 3.0)
    normals = scatter_about(splits[4], (2, DEG, NODES), 0.5, 3.0, ((2, 8),), jnp.float32)
    refract = scatter_about(splits[5], (NODES,), 0.6, 4.0, ((0, 8),), jnp.float32)
    freq_shift = scatter_about(splits[6], (NODES,), 0.6, 4.0, ((0, 8),), jnp.float32)
    nbr_list = draw_nbr_list(jax.random.fold_in(splits[10], 71), 0)
    send_nodes = draw_send_nodes(jax.random.fold_in(splits[10], 71), 0)
    adjacency = draw_adjacency(jax.random.fold_in(splits[10], 71), 0)
    return dict(action_old=action_old, source=source, time_weight=time_weight, group_speed=group_speed, normals=normals, refract=refract, freq_shift=freq_shift, nbr_list=nbr_list, send_nodes=send_nodes, adjacency=adjacency)


def reference(action_old, source, time_weight, group_speed, normals, refract, freq_shift, nbr_list, send_nodes, adjacency):
    count = nbr_list.shape[0]
    slots = nbr_list.shape[1]
    width = send_nodes.shape[2]
    local = action_old.shape[2] // count
    angles = 2.0 * math.pi * jnp.arange(DIR).astype(jnp.float32) / DIR
    cosine = jnp.cos(angles)
    sine = jnp.sin(angles)
    valid = nbr_list >= 0
    partner = jnp.where(valid, nbr_list, 0).astype(jnp.int32)
    backward = nbr_list[partner]
    subdomain = jnp.arange(count).astype(jnp.int32)
    slot_ids = jnp.arange(slots).astype(jnp.int32)
    reverse = jnp.sum(jnp.where(backward == subdomain[:, None, None], slot_ids[None, None, :], 0), axis=2).astype(jnp.int32)
    picked = send_nodes[partner, reverse]
    table = (partner[:, :, None] * local + picked).reshape(count, slots * width)
    entries = adjacency.reshape(DEG, count, local)
    position = jnp.clip(entries - local, 0, slots * width - 1)
    remote = jnp.take_along_axis(jnp.broadcast_to(table[None], (DEG, count, slots * width)), position, axis=2)
    global_index = jnp.where(entries < local, subdomain[None, :, None] * local + entries, remote)
    global_index = global_index.reshape(DEG, count * local).astype(jnp.int32)
    own_index = jnp.arange(local).astype(jnp.int32)
    used = (entries != own_index[None, None, :]).reshape(DEG, count * local)

    def flux(k):
        return group_speed[:, None, None] * (cosine[None, :, None] * normals[0, k][None, None, :] + sine[None, :, None] * normals[1, k][None, None, :])

    turning = refract[None, :] * cosine[:, None]
    diagonal = time_weight[None, None, :] + jnp.abs(turning)[None] + jnp.abs(freq_shift)[None, None, :]
    for k in range(DEG):
        diagonal = diagonal + jnp.where(used[k][None, None, :], jnp.maximum(flux(k), 0.0), 0.0)
    steady = time_weight[None, None, :] * action_old + source
    spectra = action_old
    zero_band = jnp.zeros_like(spectra[:1])
    for step in range(ITERS):
        inflow = jnp.maximum(turning, 0.0)[None] * jnp.roll(spectra, 1, axis=1) + jnp.maximum(-turning, 0.0)[None] * jnp.roll(spectra, -1, axis=1)
        lower = jnp.concatenate([zero_band, spectra[:-1]], axis=0)
        upper = jnp.concatenate([spectra[1:], zero_band], axis=0)
        inflow = inflow + jnp.maximum(freq_shift, 0.0)[None, None, :] * lower + jnp.maximum(-freq_shift, 0.0)[None, None, :] * upper
        for k in range(DEG):
            beside = jnp.take(spectra, global_index[k], axis=2)
            inflow = inflow + jnp.where(used[k][None, None, :], jnp.maximum(-flux(k), 0.0), 0.0) * beside
        spectra = (steady + inflow) / diagonal
    return spectra
```

```python
import math

import jax
import jax.numpy as jnp
import numpy as np
from jax import lax
from jax.experimental import pallas as pl
from jax.experimental.pallas import tpu as pltpu
from jax.sharding import PartitionSpec as P

REACH = 3
ITERS = 3
TILE = 256


def up_to(value, multiple):
    return -(-value // multiple) * multiple


def node_routes(count):
    masks = sorted(
        {p ^ ((p + d) % count) for p in range(count) for d in range(1, REACH + 1)}, reverse=True
    )
    reachable = all((p ^ m) < count for p in range(count) for m in masks)
    if reachable and len(masks) <= 2 * REACH:
        order = [m for m in (7, 5, 6, 3, 2, 1) if m in masks]
        order += [m for m in masks if m not in order]
        return [[p ^ m for p in range(count)] for m in order]
    routes = []
    for d in range(REACH, 0, -1):
        if count % (2 * (d & -d)) == 0 and count > 2 * d:
            for side in (0, 1):
                route = [0] * count
                for p in range(count):
                    if (p // (d & -d)) % 2 == side:
                        route[p] = (p + d) % count
                        route[(p + d) % count] = p
                routes.append(route)
        else:
            routes.append([(p + d) % count for p in range(count)])
            routes.append([(p - d) % count for p in range(count)])
    return routes


def band_routes(count):
    first = [(p ^ 1) if (p ^ 1) < count else p for p in range(count)]
    second = [p if p == 0 else p + (1 if p % 2 else -1) for p in range(count)]
    second = [q if q < count else p for p, q in enumerate(second)]
    if count % 2 == 0:
        second[0], second[-1] = count - 1, 0
    return [first, second]


def inverse(route):
    back = [0] * len(route)
    for p, q in enumerate(route):
        back[q] = p
    return back


def send(block, axis, route):
    return lax.ppermute(block, axis, list(enumerate(route)))


def split(values):
    high = values.astype(jnp.bfloat16)
    low = (values - high.astype(jnp.float32)).astype(jnp.bfloat16)
    return high, low


def hot(index, first, rows):
    ids = lax.broadcasted_iota(jnp.int32, (rows, index.shape[1]), 0) + first
    return jnp.where(ids == index, 1.0, 0.0).astype(jnp.bfloat16)


def dot(left, right, contract=((1,), (0,))):
    return lax.dot_general(left, right, (contract, ((), ())), preferred_element_type=jnp.float32)


def emit(rows_ref, chosen, flag, fields, parcels, edges, width):
    local = fields.shape[2]
    lanes = lax.broadcasted_iota(jnp.int32, (chosen.shape[0], local), 1)
    picks = jnp.where(lanes == chosen[...], 1.0, 0.0).astype(jnp.bfloat16)
    nt = ((1,), (1,))
    out = dot(picks, rows_ref[0, :, :local], nt) + dot(picks, rows_ref[1, :, :local], nt)
    for j, parcel in enumerate(parcels):
        parcel[...] = out[j * width : (j + 1) * width, :]
    last, first = fields[fields.shape[0] - 1], fields[0]
    even = flag[0] == 0
    edges[0][...] = jnp.where(even, last, first)
    edges[1][...] = jnp.where(even, first, last)


def fill_rows(rows_ref, band, values, pad):
    bands_rows = pad
    block = jnp.concatenate(
        [values, jnp.zeros((pad - values.shape[0], values.shape[1]), values.dtype)], axis=0
    )
    high, low = split(block)
    rows_ref[0, pl.ds(band * bands_rows, pad), : values.shape[1]] = high
    rows_ref[1, pl.ds(band * bands_rows, pad), : values.shape[1]] = low


def slopes(normals, trig, k, lo, hi):
    x = normals[0, k : k + 1, lo:hi]
    y = normals[1, k : k + 1, lo:hi]
    return trig[0] * x + trig[1] * y


def prep_kernel(flag, action, chosen, *refs, pad, width):
    parcels, edges, rows = refs[:-3], refs[-3:-1], refs[-1]
    bands, angles, local = action.shape
    rows[...] = jnp.zeros(rows.shape, rows.dtype)
    for f in range(bands):
        fill_rows(rows, f, action[f], pad)
    emit(rows, chosen, flag, action, parcels, edges, width)


def gathered(acc, rows, index, normals, trig, first, depth, bands, pad):
    local = index.shape[1]
    total = bands * pad
    for lo in range(0, local, TILE):
        hi = min(lo + TILE, local)
        for k in range(index.shape[0]):
            onehot = hot(index[k : k + 1, lo:hi], first, depth)
            values = dot(rows[0, :total, :depth], onehot) + dot(rows[1, :total, :depth], onehot)
            weight = jnp.maximum(-slopes(normals, trig, k, lo, hi), 0.0)
            for f in range(bands):
                piece = weight * values[f * pad : (f + 1) * pad]
                if k:
                    piece = piece + acc[f, :, lo:hi]
                acc[f, :, lo:hi] = piece


def local_kernel(speeds, *refs, pad, first):
    if first:
        (action, source, index, normals, trig_ref, nodal, part, invd, base, rows, acc) = refs
    else:
        (action, invd, base, index, normals, trig_ref, nodal, part, rows, acc) = refs
    bands, angles, local = action.shape
    trig = [jnp.broadcast_to(trig_ref[i], (pad, TILE)) for i in range(2)]
    for f in range(bands):
        fill_rows(rows, f, action[f], pad)
    gathered(acc, rows, index, normals, trig, 0, local, bands, pad)
    weight, refract, shift = nodal[0:1], nodal[1:2], nodal[2:3]
    cosine = jnp.broadcast_to(trig_ref[0], (pad, local))[:angles]
    turning = refract * cosine
    ahead, behind = jnp.maximum(turning, 0.0), jnp.maximum(-turning, 0.0)
    rising, falling = jnp.maximum(shift, 0.0), jnp.maximum(-shift, 0.0)
    if first:
        outflow = jnp.zeros((pad, local), jnp.float32)
        wide = [jnp.broadcast_to(trig_ref[i], (pad, local)) for i in range(2)]
        for k in range(index.shape[0]):
            positive = jnp.maximum(slopes(normals, wide, k, 0, local), 0.0)
            outflow = outflow + jnp.where(index[k : k + 1, :] >= 0, positive, 0.0)
        outflow = outflow[:angles]
        fixed = weight + jnp.abs(turning) + jnp.abs(shift)
    for f in range(bands):
        here = action[f]
        if first:
            inv = 1.0 / (fixed + speeds[f] * outflow)
            start = (weight * here + source[f]) * inv
            invd[f] = inv
            base[f] = start
        else:
            inv, start = invd[f], base[f]
        before = jnp.concatenate([here[angles - 1 :], here[: angles - 1]], axis=0)
        after = jnp.concatenate([here[1:], here[:1]], axis=0)
        inflow = ahead * before + behind * after + speeds[f] * acc[f, :angles, :]
        if f > 0:
            inflow = inflow + rising * action[f - 1]
        if f < bands - 1:
            inflow = inflow + falling * action[f + 1]
        part[f] = start + inflow * inv


def halo_kernel(speeds, flag, *refs, pad, width, routes, last):
    halos, refs = refs[:routes], refs[routes:]
    (edge_a, edge_b, part, invd, index, normals, trig_ref, nodal), refs = refs[:8], refs[8:]
    if last:
        out, rows, acc = refs
    else:
        chosen, out = refs[:2]
        parcels, edges, (rows, acc) = refs[2 : 2 + routes], refs[-4:-2], refs[-2:]
    bands, angles, local = part.shape
    depth = up_to(routes * width, 128)
    trig = [jnp.broadcast_to(trig_ref[i], (pad, TILE)) for i in range(2)]
    blocks = [h[...] for h in halos]
    if depth > routes * width:
        blocks.append(jnp.zeros((depth - routes * width, blocks[0].shape[1]), jnp.float32))
    received = jnp.concatenate(blocks, axis=0).T
    high, low = split(received)
    rows[0, :, :depth] = high
    rows[1, :, :depth] = low
    gathered(acc, rows, index, normals, trig, local, depth, bands, pad)
    shift = nodal[2:3]
    rising, falling = jnp.maximum(shift, 0.0), jnp.maximum(-shift, 0.0)
    even = flag[0] == 0
    below = jnp.where(flag[1] == 0, 0.0, jnp.where(even, edge_b[...], edge_a[...]))
    above = jnp.where(flag[2] == 0, 0.0, jnp.where(even, edge_a[...], edge_b[...]))
    for f in range(bands):
        inflow = speeds[f] * acc[f, :angles, :]
        if f == 0:
            inflow = inflow + rising * below
        if f == bands - 1:
            inflow = inflow + falling * above
        value = part[f] + inflow * invd[f]
        out[f] = value
        if not last:
            fill_rows(rows, f, value, pad)
    if not last:
        emit(rows, chosen, flag, out, parcels, edges, width)


def body(
    action_old,
    source,
    time_weight,
    group_speed,
    normals,
    refract,
    freq_shift,
    nbr_list,
    send_nodes,
    adjacency,
):
    bands, angles, local = action_old.shape
    slots, width = send_nodes.shape[1:]
    count = lax.axis_size("node")
    groups = lax.axis_size("freq")
    myself = lax.axis_index("node")
    band = lax.axis_index("freq")
    routes = node_routes(count)
    edge_routes = band_routes(groups)
    total = len(routes)
    pad = up_to(angles, 8)
    lanes = up_to(bands * pad, 128)
    depth = up_to(total * width, 128)

    neighbours = nbr_list[0]
    targets = jnp.asarray(np.array(routes, np.int32).T)[myself]
    sources = jnp.asarray(np.array([inverse(r) for r in routes], np.int32).T)[myself]
    match = neighbours[None, :] == targets[:, None]
    chosen = jnp.sum(jnp.where(match[:, :, None], send_nodes[0][None], 0), axis=1)
    chosen = chosen.reshape(total * width, 1)
    order = jnp.arange(total, dtype=jnp.int32)
    slot_route = jnp.sum(
        jnp.where(neighbours[:, None] == sources[None, :], order[None, :], 0), axis=1
    )
    relative = jnp.maximum(adjacency - local, 0)
    slot = relative // width
    entry_route = sum(jnp.where(slot == s, slot_route[s], 0) for s in range(slots))
    index = jnp.where(
        adjacency >= local, local + entry_route * width + relative % width, adjacency
    )
    own = jnp.arange(local, dtype=jnp.int32)
    index = jnp.where(adjacency == own[None, :], -1, index)
    theta = 2.0 * math.pi * np.arange(angles).astype(np.float32) / angles
    theta = np.concatenate([theta, np.zeros(pad - angles, np.float32)])
    trig = np.stack([np.cos(theta), np.sin(theta)]).astype(np.float32)[:, :, None]
    trig = jnp.asarray(trig)
    nodal = jnp.stack([time_weight, refract, freq_shift])
    flag = jnp.stack(
        [band % 2, (band > 0).astype(jnp.int32), (band < groups - 1).astype(jnp.int32)]
    )

    f32 = jnp.float32
    cube = jax.ShapeDtypeStruct((bands, angles, local), f32)
    parcel = jax.ShapeDtypeStruct((width, lanes), f32)
    edge = jax.ShapeDtypeStruct((angles, local), f32)
    outgoing = [parcel] * total + [edge] * 2
    rows = pltpu.VMEM((2, lanes, max(local, depth)), jnp.bfloat16)
    acc = pltpu.VMEM((bands, pad, local), f32)
    smem = pl.BlockSpec(memory_space=pltpu.SMEM)
    vmem = pl.BlockSpec(memory_space=pltpu.VMEM)
    params = pltpu.CompilerParams(vmem_limit_bytes=24 * 2**20)

    def call(kernel, scalars, arrays, outs, scratch, depth_rows, **options):
        import functools

        flops = 4 * bands * pad * depth_rows * adjacency.shape[0] * local
        return pl.pallas_call(
            functools.partial(kernel, pad=pad, **options),
            in_specs=[smem] * len(scalars) + [vmem] * len(arrays),
            out_specs=[vmem] * len(outs),
            out_shape=outs,
            scratch_shapes=scratch,
            compiler_params=params,
            cost_estimate=pl.CostEstimate(
                flops=flops, transcendentals=0, bytes_accessed=4 * bands * pad * local
            ),
        )(*scalars, *arrays)

    sends = call(prep_kernel, [flag], [action_old, chosen], outgoing, [rows], 0, width=width)
    spectra = action_old
    for step in range(ITERS):
        received = [send(x, "node", r) for x, r in zip(sends[:total], routes)]
        received += [send(x, "freq", r) for x, r in zip(sends[total:], edge_routes)]
        shared = [index, normals, trig, nodal]
        if step == 0:
            part, invd, base = call(
                local_kernel,
                [group_speed],
                [spectra, source, *shared],
                [cube] * 3,
                [rows, acc],
                local,
                first=True,
            )
        else:
            (part,) = call(
                local_kernel,
                [group_speed],
                [spectra, invd, base, *shared],
                [cube],
                [rows, acc],
                local,
                first=False,
            )
        last = step == ITERS - 1
        result = call(
            halo_kernel,
            [group_speed, flag],
            [*received, part, invd, *shared] + ([] if last else [chosen]),
            [cube] + ([] if last else outgoing),
            [rows, acc],
            depth,
            width=width,
            routes=total,
            last=last,
        )
        spectra, sends = result[0], result[1:]
    return spectra


def solution(mesh):
    in_specs = (
        P("freq", None, "node"),
        P("freq", None, "node"),
        P("node"),
        P("freq"),
        P(None, None, "node"),
        P("node"),
        P("node"),
        P("node", None),
        P("node", None, None),
        P(None, "node"),
    )
    out_specs = P("freq", None, "node")
    return jax.shard_map(body, mesh=mesh, in_specs=in_specs, out_specs=out_specs, check_vma=False)
```

```python
import functools
import math

import jax
import jax.numpy as jnp
import numpy as np
from jax import lax
from jax.experimental import pallas as pl
from jax.experimental.pallas import tpu as pltpu
from jax.sharding import PartitionSpec as P

REACH = 3
ITERS = 3
TILE = 256


def up_to(value, multiple):
    return -(-value // multiple) * multiple


def node_routes(count):
    masks = {p ^ ((p + d) % count) for p in range(count) for d in range(1, REACH + 1)}
    if count & (count - 1) == 0 and len(masks) <= 2 * REACH:
        order = [m for m in (7, 5, 6, 3, 2, 1) if m in masks]
        return [("xor", m) for m in order + sorted(masks - set(order))]
    routes = []
    for d in range(REACH, 0, -1):
        step = d & -d
        if count % (2 * step) == 0 and count > 2 * d:
            routes += [("swap", d, step, 0), ("swap", d, step, 1)]
        else:
            routes += [("shift", d), ("shift", -d)]
    return routes


def target_of(route, place, count):
    if route[0] == "xor":
        return place ^ route[1]
    if route[0] == "shift":
        return (place + route[1] + count) % count
    _, d, step, side = route
    turn = 1 - 2 * (((place // step) % 2) ^ side)
    return (place + turn * d + count) % count


def source_of(route, place, count):
    if route[0] == "shift":
        return target_of(("shift", -route[1]), place, count)
    return target_of(route, place, count)


def band_routes(count):
    first = [(p ^ 1) if (p ^ 1) < count else p for p in range(count)]
    second = [p if p == 0 else p + (1 if p % 2 else -1) for p in range(count)]
    second = [q if q < count else p for p, q in enumerate(second)]
    if count % 2 == 0:
        second[0], second[-1] = count - 1, 0
    return [first, second]


def split(values):
    high = values.astype(jnp.bfloat16)
    low = (values - high.astype(jnp.float32)).astype(jnp.bfloat16)
    return high, low


def hot(index, first, rows):
    ids = lax.broadcasted_iota(jnp.int32, (rows, index.shape[1]), 0) + first
    return jnp.where(ids == index, 1.0, 0.0).astype(jnp.bfloat16)


def dot(left, right, contract=((1,), (0,))):
    return lax.dot_general(left, right, (contract, ((), ())), preferred_element_type=jnp.float32)


def slot_with(neighbours, wanted, slots, missing):
    slot = missing
    for s in range(slots):
        slot = jnp.where(neighbours[s] == wanted, s, slot)
    return slot


def used_index(adjacency):
    index = adjacency[...]
    own = lax.broadcasted_iota(jnp.int32, index.shape, 1)
    return jnp.where(index == own, -1, index)


def store_groups(rows, get, bands, angles, unit):
    for g in range(0, bands, unit):
        values = [get(f) for f in range(g, min(g + unit, bands))]
        block = values[0] if len(values) == 1 else jnp.concatenate(values, axis=0)
        tail = up_to(block.shape[0], 8) - block.shape[0]
        if tail:
            block = jnp.concatenate([block, jnp.zeros((tail, block.shape[1]), jnp.float32)], axis=0)
        high, low = split(block)
        window = slice(g * angles, g * angles + block.shape[0])
        rows[0, window, : block.shape[1]] = high
        rows[1, window, : block.shape[1]] = low


def emit(rows, picks, flag, fields, parcels, edges, width):
    local = fields.shape[2]
    nt = ((1,), (1,))
    chosen = picks[...]
    out = dot(chosen, rows[0, :, :local], nt) + dot(chosen, rows[1, :, :local], nt)
    for j, parcel in enumerate(parcels):
        parcel[...] = out[j * width : (j + 1) * width, :]
    last, first = fields[fields.shape[0] - 1], fields[0]
    even = flag[0] == 0
    edges[0][...] = jnp.where(even, last, first)
    edges[1][...] = jnp.where(even, first, last)


def slopes(normals, trig, k, lo, hi):
    x = normals[0, k : k + 1, lo:hi]
    y = normals[1, k : k + 1, lo:hi]
    return trig[0] * x + trig[1] * y


def prep_kernel(flag, neighbours, action, sends, *refs, routes, count, unit):
    parcels, edges, picks = refs[: len(routes)], refs[-6:-4], refs[-4]
    rows, fields, arrived = refs[-3:]
    bands, angles, local = fields.shape
    slots, width = sends.shape
    copies = [
        pltpu.make_async_copy(action.at[f], fields.at[f], arrived.at[f]) for f in range(bands)
    ]
    for copy in copies:
        copy.start()
    place = flag[3]
    table = []
    for route in routes:
        slot = slot_with(neighbours, target_of(route, place, count), slots, 0)
        table.append(sends[pl.ds(slot, 1), :].astype(jnp.float32))
    height = up_to(len(routes), 8)
    if height > len(routes):
        table.append(jnp.zeros((height - len(routes), width), jnp.float32))
    table = jnp.concatenate(table, axis=0)
    if width % 128:
        spare = jnp.zeros((height, up_to(width, 128) - width), jnp.float32)
        table = jnp.concatenate([table, spare], axis=1)
    columns = table.T.astype(jnp.int32)
    lanes = lax.broadcasted_iota(jnp.int32, (width, local), 1)
    for j in range(len(routes)):
        hits = lanes == columns[:width, j : j + 1]
        picks[j * width : (j + 1) * width, :] = jnp.where(hits, 1.0, 0.0).astype(jnp.bfloat16)
    filled = bands * angles // 16 * 16
    rows[:, filled:, :] = jnp.zeros((2, rows.shape[1] - filled, rows.shape[2]), rows.dtype)

    def get(f):
        copies[f].wait()
        return fields[f]

    store_groups(rows, get, bands, angles, unit)
    emit(rows, picks, flag, fields, parcels, edges, width)


def gathered(acc, rows, index, normals, trig, first, depth, bands, angles, unit):
    local = index.shape[1]
    total = up_to(bands * angles, 8)
    for lo in range(0, local, TILE):
        hi = min(lo + TILE, local)
        for k in range(index.shape[0]):
            onehot = hot(index[k : k + 1, lo:hi], first, depth)
            values = dot(rows[0, :total, :depth], onehot) + dot(rows[1, :total, :depth], onehot)
            weight = jnp.maximum(-slopes(normals, trig, k, lo, hi), 0.0)
            for g in range(0, bands, unit):
                height = up_to(min(unit, bands - g) * angles, 8)
                window = slice(g * angles, g * angles + height)
                piece = weight[:height] * values[window]
                if k:
                    piece = piece + acc[window, lo:hi]
                acc[window, lo:hi] = piece


def local_kernel(speeds, *refs, first, unit):
    if first:
        (action, source_hbm, adjacency, normals, trig_ref, weight, refract, shift) = refs[:8]
        part, invd, base, rows, acc, source, arrived = refs[8:]
        copy = pltpu.make_async_copy(source_hbm, source, arrived)
        copy.start()
    else:
        (action, invd, base, adjacency, normals, trig_ref, weight, refract, shift) = refs[:9]
        part, rows, acc = refs[9:]
    bands, angles, local = action.shape
    index = used_index(adjacency)
    height = trig_ref.shape[1]
    trig = [jnp.broadcast_to(trig_ref[i], (height, TILE)) for i in range(2)]
    store_groups(rows, lambda f: action[f], bands, angles, unit)
    gathered(acc, rows, index, normals, trig, 0, local, bands, angles, unit)
    cosine = jnp.broadcast_to(trig_ref[0, :angles], (angles, local))
    turning = refract[...] * cosine
    ahead, behind = jnp.maximum(turning, 0.0), jnp.maximum(-turning, 0.0)
    rising, falling = jnp.maximum(shift[...], 0.0), jnp.maximum(-shift[...], 0.0)
    if first:
        outflow = jnp.zeros((angles, local), jnp.float32)
        wide = [jnp.broadcast_to(trig_ref[i, :angles], (angles, local)) for i in range(2)]
        for k in range(index.shape[0]):
            positive = jnp.maximum(slopes(normals, wide, k, 0, local), 0.0)
            outflow = outflow + jnp.where(index[k : k + 1, :] >= 0, positive, 0.0)
        fixed = weight[...] + jnp.abs(turning) + jnp.abs(shift[...])
        copy.wait()
    for f in range(bands):
        here = action[f]
        if first:
            inv = 1.0 / (fixed + speeds[f] * outflow)
            start = (weight[...] * here + source[f]) * inv
            invd[f] = inv
            base[f] = start
        else:
            inv, start = invd[f], base[f]
        before = jnp.concatenate([here[angles - 1 :], here[: angles - 1]], axis=0)
        after = jnp.concatenate([here[1:], here[:1]], axis=0)
        edges = acc[f * angles : (f + 1) * angles, :]
        inflow = ahead * before + behind * after + speeds[f] * edges
        if f > 0:
            inflow = inflow + rising * action[f - 1]
        if f < bands - 1:
            inflow = inflow + falling * action[f + 1]
        part[f] = start + inflow * inv


def halo_kernel(speeds, flag, neighbours, *refs, routes, count, width, last, unit):
    total = len(routes)
    halos, refs = refs[:total], refs[total:]
    (edge_a, edge_b, part, invd, adjacency, normals, trig_ref, shift), refs = refs[:8], refs[8:]
    if last:
        out, rows, acc, inbox = refs
    else:
        picks, out = refs[:2]
        parcels, edges, (rows, acc, inbox) = refs[2 : 2 + total], refs[-5:-3], refs[-3:]
    bands, angles, local = part.shape
    slots = neighbours.shape[0]
    depth = inbox.shape[0]
    index = used_index(adjacency)
    trig = [jnp.broadcast_to(trig_ref[i], (trig_ref.shape[1], TILE)) for i in range(2)]
    inbox[...] = jnp.zeros(inbox.shape, inbox.dtype)
    for route, halo in zip(routes, halos):
        slot = slot_with(neighbours, source_of(route, flag[3], count), slots, slots)
        inbox[pl.ds(pl.multiple_of(slot * width, width), width), :] = halo[...]
    high, low = split(inbox[...].T)
    rows[0, :, :depth] = high
    rows[1, :, :depth] = low
    gathered(acc, rows, index, normals, trig, local, depth, bands, angles, unit)
    rising, falling = jnp.maximum(shift[...], 0.0), jnp.maximum(-shift[...], 0.0)
    even = flag[0] == 0
    below = jnp.where(flag[1] == 0, 0.0, jnp.where(even, edge_b[...], edge_a[...]))
    above = jnp.where(flag[2] == 0, 0.0, jnp.where(even, edge_a[...], edge_b[...]))

    def get(f):
        inflow = speeds[f] * acc[f * angles : (f + 1) * angles, :]
        if f == 0:
            inflow = inflow + rising * below
        if f == bands - 1:
            inflow = inflow + falling * above
        value = part[f] + inflow * invd[f]
        out[f] = value
        return value

    if last:
        for f in range(bands):
            get(f)
    else:
        filled = bands * angles // 16 * 16
        rows[:, filled:, :] = jnp.zeros((2, rows.shape[1] - filled, rows.shape[2]), rows.dtype)
        store_groups(rows, get, bands, angles, unit)
        emit(rows, picks, flag, out, parcels, edges, width)


def body(
    action_old,
    source,
    time_weight,
    group_speed,
    normals,
    refract,
    freq_shift,
    nbr_list,
    send_nodes,
    adjacency,
):
    bands, angles, local = action_old.shape
    slots, width = send_nodes.shape[1:]
    count = lax.axis_size("node")
    groups = lax.axis_size("freq")
    myself = lax.axis_index("node")
    band = lax.axis_index("freq")
    routes = node_routes(count)
    edge_routes = band_routes(groups)
    total = len(routes)
    unit = 8 // math.gcd(angles, 8)
    lanes = up_to(bands * angles, 128)
    depth = up_to((slots + 1) * width, 128)

    theta = 2.0 * math.pi * np.arange(angles).astype(np.float32) / angles
    trig = np.stack([np.cos(theta), np.sin(theta)]).astype(np.float32)[:, :, None]
    trig = jnp.asarray(np.concatenate([trig] * unit, axis=1))
    flag = jnp.stack(
        [band % 2, (band > 0).astype(jnp.int32), (band < groups - 1).astype(jnp.int32), myself]
    )
    neighbours = nbr_list.reshape(slots)

    f32 = jnp.float32
    cube = jax.ShapeDtypeStruct((bands, angles, local), f32)
    parcel = jax.ShapeDtypeStruct((width, lanes), f32)
    edge = jax.ShapeDtypeStruct((angles, local), f32)
    chosen = jax.ShapeDtypeStruct((total * width, local), jnp.bfloat16)
    outgoing = [parcel] * total + [edge] * 2
    rows = pltpu.VMEM((2, lanes, max(local, depth)), jnp.bfloat16)
    acc = pltpu.VMEM((up_to(bands * angles, 8), local), f32)
    inbox = pltpu.VMEM((depth, lanes), f32)
    fields = pltpu.VMEM((bands, angles, local), f32)
    smem = pl.BlockSpec(memory_space=pltpu.SMEM)
    vmem = pl.BlockSpec(memory_space=pltpu.VMEM)
    anywhere = pl.BlockSpec(memory_space=pl.ANY)
    params = pltpu.CompilerParams(vmem_limit_bytes=24 * 2**20)

    def call(kernel, scalars, arrays, outs, scratch, depth_rows, far=None, **options):
        flops = 4 * bands * angles * depth_rows * adjacency.shape[0] * local
        specs = [smem] * len(scalars) + [vmem] * len(arrays)
        if far is not None:
            specs[len(scalars) + far] = anywhere
        return pl.pallas_call(
            functools.partial(kernel, unit=unit, **options),
            in_specs=specs,
            out_specs=[vmem] * len(outs),
            out_shape=outs,
            scratch_shapes=scratch,
            compiler_params=params,
            cost_estimate=pl.CostEstimate(
                flops=flops, transcendentals=0, bytes_accessed=4 * bands * angles * local
            ),
        )(*scalars, *arrays)

    *sends, picks = call(
        prep_kernel,
        [flag, neighbours],
        [action_old, send_nodes.reshape(slots, width)],
        outgoing + [chosen],
        [rows, fields, pltpu.SemaphoreType.DMA((bands,))],
        0,
        far=0,
        routes=routes,
        count=count,
    )
    nodal = [x.reshape(1, local) for x in (time_weight, refract, freq_shift)]
    spectra = action_old
    for step in range(ITERS):
        received = [
            lax.ppermute(x, "node", [(p, target_of(r, p, count)) for p in range(count)])
            for x, r in zip(sends[:total], routes)
        ]
        received += [
            lax.ppermute(x, "freq", list(enumerate(r)))
            for x, r in zip(sends[total:], edge_routes)
        ]
        shared = [adjacency, normals, trig]
        if step == 0:
            part, invd, base = call(
                local_kernel,
                [group_speed],
                [spectra, source, *shared, *nodal],
                [cube] * 3,
                [rows, acc, fields, pltpu.SemaphoreType.DMA],
                local,
                far=1,
                first=True,
            )
        else:
            (part,) = call(
                local_kernel,
                [group_speed],
                [spectra, invd, base, *shared, *nodal],
                [cube],
                [rows, acc],
                local,
                first=False,
            )
        last = step == ITERS - 1
        spectra, *sends = call(
            halo_kernel,
            [group_speed, flag, neighbours],
            [*received, part, invd, *shared, nodal[2]] + ([] if last else [picks]),
            [cube] + ([] if last else outgoing),
            [rows, acc, inbox],
            depth,
            routes=routes,
            count=count,
            width=width,
            last=last,
        )
    return spectra


def solution(mesh):
    in_specs = (
        P("freq", None, "node"),
        P("freq", None, "node"),
        P("node"),
        P("freq"),
        P(None, None, "node"),
        P("node"),
        P("node"),
        P("node", None),
        P("node", None, None),
        P(None, "node"),
    )
    out_specs = P("freq", None, "node")
    return jax.shard_map(body, mesh=mesh, in_specs=in_specs, out_specs=out_specs, check_vma=False)
```

```python
import functools
import math

import jax
import jax.numpy as jnp
import numpy as np
from jax import lax
from jax.experimental import pallas as pl
from jax.experimental.pallas import tpu as pltpu
from jax.sharding import PartitionSpec as P

REACH = 3
ITERS = 3
TILE = 256


def up_to(value, multiple):
    return -(-value // multiple) * multiple


def node_routes(count):
    masks = {p ^ ((p + d) % count) for p in range(count) for d in range(1, REACH + 1)}
    if count & (count - 1) == 0 and len(masks) <= 2 * REACH:
        order = [m for m in (7, 5, 6, 3, 2, 1) if m in masks]
        return [("xor", m) for m in order + sorted(masks - set(order))]
    routes = []
    for d in range(REACH, 0, -1):
        step = d & -d
        if count % (2 * step) == 0 and count > 2 * d:
            routes += [("swap", d, step, 0), ("swap", d, step, 1)]
        else:
            routes += [("shift", d), ("shift", -d)]
    return routes


def target_of(route, place, count):
    if route[0] == "xor":
        return place ^ route[1]
    if route[0] == "shift":
        return (place + route[1] + count) % count
    _, d, step, side = route
    turn = 1 - 2 * (((place // step) % 2) ^ side)
    return (place + turn * d + count) % count


def source_of(route, place, count):
    if route[0] == "shift":
        return target_of(("shift", -route[1]), place, count)
    return target_of(route, place, count)


def band_routes(count):
    first = [(p ^ 1) if (p ^ 1) < count else p for p in range(count)]
    second = [p if p == 0 else p + (1 if p % 2 else -1) for p in range(count)]
    second = [q if q < count else p for p, q in enumerate(second)]
    if count % 2 == 0:
        second[0], second[-1] = count - 1, 0
    return [first, second]


def split(values):
    high = values.astype(jnp.bfloat16)
    low = (values - high.astype(jnp.float32)).astype(jnp.bfloat16)
    return high, low


def hot(index, first, rows):
    ids = lax.broadcasted_iota(jnp.int32, (rows, index.shape[1]), 0) + first
    return jnp.where(ids == index, 1.0, 0.0).astype(jnp.bfloat16)


def dot(left, right, contract=((1,), (0,))):
    return lax.dot_general(left, right, (contract, ((), ())), preferred_element_type=jnp.float32)


def store_groups(rows, get, bands, angles, unit):
    for g in range(0, bands, unit):
        values = [get(f) for f in range(g, min(g + unit, bands))]
        block = values[0] if len(values) == 1 else jnp.concatenate(values, axis=0)
        tail = up_to(block.shape[0], 8) - block.shape[0]
        if tail:
            block = jnp.concatenate([block, jnp.zeros((tail, block.shape[1]), jnp.float32)], axis=0)
        high, low = split(block)
        window = slice(g * angles, g * angles + block.shape[0])
        rows[0, window, : block.shape[1]] = high
        rows[1, window, : block.shape[1]] = low


def emit(rows, picks, even, fields, parcels, edges, width):
    local = fields.shape[2]
    nt = ((1,), (1,))
    chosen = picks[...]
    out = dot(chosen, rows[0, :, :local], nt) + dot(chosen, rows[1, :, :local], nt)
    for j, parcel in enumerate(parcels):
        parcel[...] = out[j * width : (j + 1) * width, :]
    last, first = fields[fields.shape[0] - 1], fields[0]
    edges[0][...] = jnp.where(even, last, first)
    edges[1][...] = jnp.where(even, first, last)


def clear_tail(rows, used):
    start = used // 16 * 16
    rows[:, start:, :] = jnp.zeros((2, rows.shape[1] - start, rows.shape[2]), rows.dtype)


def slopes(normals, trig, k, lo, hi):
    x = normals[0, k : k + 1, lo:hi]
    y = normals[1, k : k + 1, lo:hi]
    return trig[0] * x + trig[1] * y


WEIGHT, REFRACT, SHIFT, EVEN, RISE, FALL, TABLE = 0, 1, 2, 3, 4, 5, 8


def prep_kernel(
    action, near, sends_in, adjacency_in, normals_in, weight, refract, shift, trig_in, *refs, routes, axes, unit
):
    node, freq, count, groups = axes
    total = len(routes)
    parcels, edges, refs = refs[:total], refs[total : total + 2], refs[total + 2 :]
    picks, fields, index_out, normals, nodal, trig = refs[:6]
    rows, neighbours, sends, adjacency, raw, line, arrived, small = refs[6:]
    bands, angles, local = fields.shape
    slots, width = sends.shape[0], sends.shape[2]
    pairs = [
        (near, neighbours),
        (sends_in, sends),
        (adjacency_in, adjacency),
        (normals_in, raw),
        (weight, nodal.at[pl.ds(WEIGHT, 1)]),
        (refract, nodal.at[pl.ds(REFRACT, 1)]),
        (shift, nodal.at[pl.ds(SHIFT, 1)]),
        (trig_in, line),
    ]
    little = [pltpu.make_async_copy(x, y, small.at[i]) for i, (x, y) in enumerate(pairs)]
    copies = [
        pltpu.make_async_copy(action.at[f], fields.at[f], arrived.at[f]) for f in range(bands)
    ]
    for copy in little[:2] + copies + little[2:]:
        copy.start()
    place, band = lax.axis_index(node), lax.axis_index(freq)
    clear_tail(rows, bands * angles)
    for copy in little[:2]:
        copy.wait()
    near_of = [neighbours[0, s] for s in range(slots)]
    table = []
    for route in routes:
        target = target_of(route, place, count)
        slot = jnp.int32(0)
        for s in range(slots):
            slot = jnp.where(near_of[s] == target, s, slot)
        table.append(sends[slot].astype(jnp.float32))
    height = up_to(total, 8)
    if height > total:
        table.append(jnp.zeros((height - total, width), jnp.float32))
    table = jnp.concatenate(table, axis=0)
    if width % 128:
        spare = jnp.zeros((height, up_to(width, 128) - width), jnp.float32)
        table = jnp.concatenate([table, spare], axis=1)
    columns = table.T.astype(jnp.int32)
    lanes = lax.broadcasted_iota(jnp.int32, (width, local), 1)
    for j in range(total):
        hits = lanes == columns[:width, j : j + 1]
        picks[j * width : (j + 1) * width, :] = jnp.where(hits, 1.0, 0.0).astype(jnp.bfloat16)

    def get(f):
        copies[f].wait()
        return fields[f]

    store_groups(rows, get, bands, angles, unit)
    is_even = jnp.full((1, local), band % 2, jnp.int32) == 0
    emit(rows, picks, is_even, fields, parcels, edges, width)
    for copy in little[2:]:
        copy.wait()
    entry = adjacency[...]
    index = entry
    for s in range(slots):
        route = jnp.int32(0)
        for j, r in enumerate(routes):
            route = jnp.where(near_of[s] == source_of(r, place, count), j, route)
        inside = (entry >= local + s * width) & (entry < local + (s + 1) * width)
        index = jnp.where(inside, entry + (route - s) * width, index)
    index_out[...] = index
    used = entry != lax.broadcasted_iota(jnp.int32, entry.shape, 1)
    for i in range(2):
        normals[i] = jnp.where(used, raw[i], 0.0)
        trig[i] = jnp.broadcast_to(line[i], trig.shape[1:])
    moved = nodal[SHIFT : SHIFT + 1]
    has_below = jnp.where(band > 0, 1.0, 0.0)
    has_above = jnp.where(band < groups - 1, 1.0, 0.0)
    nodal[EVEN : EVEN + 1] = jnp.where(is_even, 1.0, 0.0)
    nodal[RISE : RISE + 1] = jnp.maximum(moved, 0.0) * has_below
    nodal[FALL : FALL + 1] = jnp.maximum(-moved, 0.0) * has_above
    nodal[FALL + 1 :] = jnp.zeros((TABLE - FALL - 1, local), jnp.float32)


def gathered(acc, rows, index, normals, trig, first, depth, bands, angles, unit, finish):
    local = index.shape[1]
    total = up_to(bands * angles, 8)
    waiting = []
    for lo in range(0, local, TILE):
        hi = min(lo + TILE, local)
        for k in range(index.shape[0]):
            onehot = hot(index[k : k + 1, lo:hi], first, depth)
            values = dot(rows[0, :total, :depth], onehot) + dot(rows[1, :total, :depth], onehot)
            weight = jnp.maximum(-slopes(normals, trig, k, lo, hi), 0.0)
            for g in range(0, bands, unit):
                height = up_to(min(unit, bands - g) * angles, 8)
                window = slice(g * angles, g * angles + height)
                piece = weight[:height] * values[window]
                if k:
                    piece = piece + acc[window, lo:hi]
                acc[window, lo:hi] = piece
            for _ in range(-(-bands // index.shape[0])):
                if waiting:
                    finish(*waiting.pop(0))
        for item in waiting:
            finish(*item)
        waiting = [(f, lo, hi) for f in range(bands)]
    for item in waiting:
        finish(*item)


def local_kernel(*refs, first, unit):
    if first:
        (action, source_hbm, speeds_hbm, index, normals, nodal, trig) = refs[:7]
        part, invd, invs, base, rows, acc, source, speeds, arrived, came = refs[7:]
        copy = pltpu.make_async_copy(source_hbm, source, arrived)
        copy.start()
        fetch = pltpu.make_async_copy(speeds_hbm, speeds, came)
        fetch.start()
    else:
        (action, invd, invs, base, index, normals, nodal, trig) = refs[:8]
        part, rows, acc = refs[8:]
    bands, angles, local = action.shape
    store_groups(rows, lambda f: action[f], bands, angles, unit)
    if first:
        copy.wait()
        fetch.wait()

    def finish(f, lo, hi):
        here = action[f, :, lo:hi]
        shift = nodal[SHIFT : SHIFT + 1, lo:hi]
        turning = nodal[REFRACT : REFRACT + 1, lo:hi] * trig[0, :angles, : hi - lo]
        if first:
            outflow = jnp.zeros((angles, hi - lo), jnp.float32)
            wave = [trig[i, :angles, : hi - lo] for i in range(2)]
            weight = nodal[WEIGHT : WEIGHT + 1, lo:hi]
            if f == 0:
                for k in range(index.shape[0]):
                    outflow = outflow + jnp.maximum(slopes(normals, wave, k, lo, hi), 0.0)
                kept[lo] = (outflow, weight + jnp.abs(turning) + jnp.abs(shift))
            outflow, fixed = kept[lo]
            inv = 1.0 / (fixed + speeds[0, f] * outflow)
            start = (weight * here + source[f, :, lo:hi]) * inv
            scaled = speeds[0, f] * inv
            invd[f, :, lo:hi] = inv
            invs[f, :, lo:hi] = scaled
            base[f, :, lo:hi] = start
        else:
            inv, scaled, start = invd[f, :, lo:hi], invs[f, :, lo:hi], base[f, :, lo:hi]
        before = jnp.concatenate([here[angles - 1 :], here[: angles - 1]], axis=0)
        after = jnp.concatenate([here[1:], here[:1]], axis=0)
        inflow = jnp.maximum(turning, 0.0) * before + jnp.maximum(-turning, 0.0) * after
        if f > 0:
            inflow = inflow + jnp.maximum(shift, 0.0) * action[f - 1, :, lo:hi]
        if f < bands - 1:
            inflow = inflow + jnp.maximum(-shift, 0.0) * action[f + 1, :, lo:hi]
        edges = acc[f * angles : (f + 1) * angles, lo:hi]
        part[f, :, lo:hi] = start + inflow * inv + edges * scaled

    kept = {}
    gathered(acc, rows, index, normals, trig, 0, local, bands, angles, unit, finish)


def halo_kernel(*refs, routes, width, last, unit):
    halos, refs = refs[:routes], refs[routes:]
    (edge_a, edge_b, part, invd, invs, index, normals, nodal, trig), refs = refs[:9], refs[9:]
    if last:
        out, rows, acc = refs
    else:
        picks, out = refs[:2]
        parcels, edges, (rows, acc) = refs[2 : 2 + routes], refs[-4:-2], refs[-2:]
    bands, angles, local = part.shape
    depth = up_to(routes * width, 128)
    blocks = [halo[...] for halo in halos]
    if depth > routes * width:
        blocks.append(jnp.zeros((depth - routes * width, blocks[0].shape[1]), jnp.float32))
    high, low = split(jnp.concatenate(blocks, axis=0).T)
    rows[0, :, :depth] = high
    rows[1, :, :depth] = low
    is_even = nodal[EVEN : EVEN + 1, :] > 0.5

    def finish(f, lo, hi):
        value = part[f, :, lo:hi] + acc[f * angles : (f + 1) * angles, lo:hi] * invs[f, :, lo:hi]
        even = is_even[:, lo:hi]
        if f == 0:
            below = jnp.where(even, edge_b[:, lo:hi], edge_a[:, lo:hi])
            value = value + nodal[RISE : RISE + 1, lo:hi] * below * invd[f, :, lo:hi]
        if f == bands - 1:
            above = jnp.where(even, edge_a[:, lo:hi], edge_b[:, lo:hi])
            value = value + nodal[FALL : FALL + 1, lo:hi] * above * invd[f, :, lo:hi]
        out[f, :, lo:hi] = value

    gathered(acc, rows, index, normals, trig, local, depth, bands, angles, unit, finish)
    if not last:
        clear_tail(rows, bands * angles)
        store_groups(rows, lambda f: out[f], bands, angles, unit)
        emit(rows, picks, is_even, out, parcels, edges, width)


def body(
    action_old,
    source,
    time_weight,
    group_speed,
    normals,
    refract,
    freq_shift,
    nbr_list,
    send_nodes,
    adjacency,
):
    bands, angles, local = action_old.shape
    slots, width = send_nodes.shape[1:]
    degree = adjacency.shape[0]
    count = lax.axis_size("node")
    groups = lax.axis_size("freq")
    routes = node_routes(count)
    edge_routes = band_routes(groups)
    total = len(routes)
    unit = 8 // math.gcd(angles, 8)
    lanes = up_to(bands * angles, 128)
    depth = up_to(total * width, 128)

    theta = 2.0 * math.pi * np.arange(angles).astype(np.float32) / angles
    trig = np.stack([np.cos(theta), np.sin(theta)]).astype(np.float32)[:, :, None]
    trig = jnp.asarray(np.concatenate([trig] * unit, axis=1))

    f32, i32, bf16 = jnp.float32, jnp.int32, jnp.bfloat16
    shape = jax.ShapeDtypeStruct
    cube = shape((bands, angles, local), f32)
    outgoing = [shape((width, lanes), f32)] * total + [shape((angles, local), f32)] * 2
    tables = [
        shape((total * width, local), bf16),
        cube,
        shape((degree, local), i32),
        shape((2, degree, local), f32),
        shape((TABLE, local), f32),
        shape((2, unit * angles, TILE), f32),
    ]
    rows = pltpu.VMEM((2, lanes, max(local, depth)), bf16)
    acc = pltpu.VMEM((up_to(bands * angles, 8), local), f32)
    dma = pltpu.SemaphoreType.DMA
    vmem = pl.BlockSpec(memory_space=pltpu.VMEM)
    far = pl.BlockSpec(memory_space=pltpu.HBM)
    params = pltpu.CompilerParams(vmem_limit_bytes=24 * 2**20)

    def call(kernel, arrays, outs, scratch, depth_rows, distant=(), **options):
        flops = 4 * bands * angles * depth_rows * degree * local
        return pl.pallas_call(
            functools.partial(kernel, unit=unit, **options),
            in_specs=[far if i in distant else vmem for i in range(len(arrays))],
            out_specs=[vmem] * len(outs),
            out_shape=outs,
            scratch_shapes=scratch,
            compiler_params=params,
            cost_estimate=pl.CostEstimate(
                flops=flops, transcendentals=0, bytes_accessed=4 * bands * angles * local
            ),
        )(*arrays)

    nodal = [x.reshape(1, local) for x in (time_weight, refract, freq_shift)]
    prepared = call(
        prep_kernel,
        [action_old, nbr_list, send_nodes.reshape(slots, 1, width), adjacency, normals, *nodal, trig],
        outgoing + tables,
        [
            rows,
            pltpu.SMEM((1, slots), i32),
            pltpu.VMEM((slots, 1, width), i32),
            pltpu.VMEM((degree, local), i32),
            pltpu.VMEM((2, degree, local), f32),
            pltpu.VMEM(trig.shape, f32),
            dma((bands,)),
            dma((8,)),
        ],
        0,
        distant=range(9),
        routes=routes,
        axes=("node", "freq", count, groups),
    )
    sends = prepared[: total + 2]
    picks, spectra, *shared = prepared[total + 2 :]
    for step in range(ITERS):
        received = [
            lax.ppermute(x, "node", [(p, target_of(r, p, count)) for p in range(count)])
            for x, r in zip(sends[:total], routes)
        ]
        received += [
            lax.ppermute(x, "freq", list(enumerate(r)))
            for x, r in zip(sends[total:], edge_routes)
        ]
        if step == 0:
            part, invd, invs, base = call(
                local_kernel,
                [spectra, source, group_speed.reshape(1, bands), *shared],
                [cube] * 4,
                [
                    rows,
                    acc,
                    pltpu.VMEM((bands, angles, local), f32),
                    pltpu.SMEM((1, bands), f32),
                    dma,
                    dma,
                ],
                local,
                distant=(1, 2),
                first=True,
            )
        else:
            (part,) = call(
                local_kernel,
                [spectra, invd, invs, base, *shared],
                [cube],
                [rows, acc],
                local,
                first=False,
            )
        last = step == ITERS - 1
        spectra, *sends = call(
            halo_kernel,
            [*received, part, invd, invs, *shared] + ([] if last else [picks]),
            [cube] + ([] if last else outgoing),
            [rows, acc],
            depth,
            routes=total,
            width=width,
            last=last,
        )
    return spectra


def solution(mesh):
    in_specs = (
        P("freq", None, "node"),
        P("freq", None, "node"),
        P("node"),
        P("freq"),
        P(None, None, "node"),
        P("node"),
        P("node"),
        P("node", None),
        P("node", None, None),
        P(None, "node"),
    )
    out_specs = P("freq", None, "node")
    return jax.shard_map(body, mesh=mesh, in_specs=in_specs, out_specs=out_specs, check_vma=False)
```

```python
import functools
import math

import jax
import jax.numpy as jnp
import numpy as np
from jax import lax
from jax.experimental import pallas as pl
from jax.experimental.pallas import tpu as pltpu
from jax.sharding import PartitionSpec as P

REACH = 3
ITERS = 3
TILE = 256


def up_to(value, multiple):
    return -(-value // multiple) * multiple


def node_routes(count):
    masks = {p ^ ((p + d) % count) for p in range(count) for d in range(1, REACH + 1)}
    if count & (count - 1) == 0 and len(masks) <= 2 * REACH:
        order = [m for m in (7, 5, 6, 3, 2, 1) if m in masks]
        return [("xor", m) for m in order + sorted(masks - set(order))]
    routes = []
    for d in range(REACH, 0, -1):
        step = d & -d
        if count % (2 * step) == 0 and count > 2 * d:
            routes += [("swap", d, step, 0), ("swap", d, step, 1)]
        else:
            routes += [("shift", d), ("shift", -d)]
    return routes


def target_of(route, place, count):
    if route[0] == "xor":
        return place ^ route[1]
    if route[0] == "shift":
        return (place + route[1] + count) % count
    _, d, step, side = route
    turn = 1 - 2 * (((place // step) % 2) ^ side)
    return (place + turn * d + count) % count


def source_of(route, place, count):
    if route[0] == "shift":
        return target_of(("shift", -route[1]), place, count)
    return target_of(route, place, count)


def band_routes(count):
    first = [(p ^ 1) if (p ^ 1) < count else p for p in range(count)]
    second = [p if p == 0 else p + (1 if p % 2 else -1) for p in range(count)]
    second = [q if q < count else p for p, q in enumerate(second)]
    if count % 2 == 0:
        second[0], second[-1] = count - 1, 0
    return [first, second]


def split(values):
    high = values.astype(jnp.bfloat16)
    low = (values - high.astype(jnp.float32)).astype(jnp.bfloat16)
    return high, low


def hot(index, first, rows):
    ids = lax.broadcasted_iota(jnp.int32, (rows, index.shape[1]), 0) + first
    return jnp.where(ids == index, 1.0, 0.0).astype(jnp.bfloat16)


def dot(left, right, contract=((1,), (0,))):
    return lax.dot_general(left, right, (contract, ((), ())), preferred_element_type=jnp.float32)


def store_groups(rows, get, bands, angles, unit):
    for g in range(0, bands, unit):
        values = [get(f) for f in range(g, min(g + unit, bands))]
        block = values[0] if len(values) == 1 else jnp.concatenate(values, axis=0)
        tail = up_to(block.shape[0], 8) - block.shape[0]
        if tail:
            block = jnp.concatenate([block, jnp.zeros((tail, block.shape[1]), jnp.float32)], axis=0)
        high, low = split(block)
        window = slice(g * angles, g * angles + block.shape[0])
        rows[0, window, : block.shape[1]] = high
        rows[1, window, : block.shape[1]] = low


def emit(rows, picks, even, fields, parcels, edges, width):
    local = fields.shape[2]
    nt = ((1,), (1,))
    chosen = picks[...]
    out = dot(chosen, rows[0, :, :local], nt) + dot(chosen, rows[1, :, :local], nt)
    for j, parcel in enumerate(parcels):
        parcel[...] = out[j * width : (j + 1) * width, :]
    last, first = fields[fields.shape[0] - 1], fields[0]
    edges[0][...] = jnp.where(even, last, first)
    edges[1][...] = jnp.where(even, first, last)


def clear_tail(rows, used):
    start = used // 16 * 16
    rows[:, start:, :] = jnp.zeros((2, rows.shape[1] - start, rows.shape[2]), rows.dtype)


def slopes(normals, trig, k, lo, hi):
    x = normals[0, k : k + 1, lo:hi]
    y = normals[1, k : k + 1, lo:hi]
    return trig[0] * x + trig[1] * y


WEIGHT, REFRACT, SHIFT, EVEN, RISE, FALL, TABLE = 0, 1, 2, 3, 4, 5, 8


def prep_kernel(
    action, near, sends_in, adjacency_in, normals_in, weight, refract, shift, trig_in, *refs, routes, axes, unit
):
    node, freq, count, groups = axes
    total = len(routes)
    parcels, edges, refs = refs[:total], refs[total : total + 2], refs[total + 2 :]
    picks, fields, index_out, normals, nodal, trig = refs[:6]
    rows, neighbours, sends, adjacency, raw, line, arrived, small = refs[6:]
    bands, angles, local = fields.shape
    slots, width = sends.shape[0], sends.shape[2]
    pairs = [
        (near, neighbours),
        (sends_in, sends),
        (adjacency_in, adjacency),
        (normals_in, raw),
        (weight, nodal.at[pl.ds(WEIGHT, 1)]),
        (refract, nodal.at[pl.ds(REFRACT, 1)]),
        (shift, nodal.at[pl.ds(SHIFT, 1)]),
        (trig_in, line),
    ]
    little = [pltpu.make_async_copy(x, y, small.at[i]) for i, (x, y) in enumerate(pairs)]
    copies = [
        pltpu.make_async_copy(action.at[f], fields.at[f], arrived.at[f]) for f in range(bands)
    ]
    for copy in little[:2] + copies + little[2:]:
        copy.start()
    place, band = lax.axis_index(node), lax.axis_index(freq)
    clear_tail(rows, bands * angles)
    for copy in little[:2]:
        copy.wait()
    near_of = [neighbours[0, s] for s in range(slots)]
    table = []
    for route in routes:
        target = target_of(route, place, count)
        slot = jnp.int32(0)
        for s in range(slots):
            slot = jnp.where(near_of[s] == target, s, slot)
        table.append(sends[slot].astype(jnp.float32))
    height = up_to(total, 8)
    if height > total:
        table.append(jnp.zeros((height - total, width), jnp.float32))
    table = jnp.concatenate(table, axis=0)
    if width % 128:
        spare = jnp.zeros((height, up_to(width, 128) - width), jnp.float32)
        table = jnp.concatenate([table, spare], axis=1)
    columns = table.T.astype(jnp.int32)
    lanes = lax.broadcasted_iota(jnp.int32, (width, local), 1)
    for j in range(total):
        hits = lanes == columns[:width, j : j + 1]
        picks[j * width : (j + 1) * width, :] = jnp.where(hits, 1.0, 0.0).astype(jnp.bfloat16)

    def get(f):
        copies[f].wait()
        return fields[f]

    store_groups(rows, get, bands, angles, unit)
    is_even = jnp.full((1, local), band % 2, jnp.int32) == 0
    emit(rows, picks, is_even, fields, parcels, edges, width)
    for copy in little[2:]:
        copy.wait()
    entry = adjacency[...]
    index = entry
    for s in range(slots):
        route = jnp.int32(0)
        for j, r in enumerate(routes):
            route = jnp.where(near_of[s] == source_of(r, place, count), j, route)
        inside = (entry >= local + s * width) & (entry < local + (s + 1) * width)
        index = jnp.where(inside, entry + (route - s) * width, index)
    index_out[...] = index
    used = entry != lax.broadcasted_iota(jnp.int32, entry.shape, 1)
    for i in range(2):
        normals[i] = jnp.where(used, raw[i], 0.0)
        trig[i] = jnp.broadcast_to(line[i], trig.shape[1:])
    moved = nodal[SHIFT : SHIFT + 1]
    has_below = jnp.where(band > 0, 1.0, 0.0)
    has_above = jnp.where(band < groups - 1, 1.0, 0.0)
    nodal[EVEN : EVEN + 1] = jnp.where(is_even, 1.0, 0.0)
    nodal[RISE : RISE + 1] = jnp.maximum(moved, 0.0) * has_below
    nodal[FALL : FALL + 1] = jnp.maximum(-moved, 0.0) * has_above
    nodal[FALL + 1 :] = jnp.zeros((TABLE - FALL - 1, local), jnp.float32)


def gathered(acc, rows, index, normals, trig, first, depth, bands, angles, unit, finish):
    local = index.shape[1]
    total = up_to(bands * angles, 8)
    waiting = []
    for lo in range(0, local, TILE):
        hi = min(lo + TILE, local)
        for k in range(index.shape[0]):
            onehot = hot(index[k : k + 1, lo:hi], first, depth)
            values = dot(rows[0, :total, :depth], onehot) + dot(rows[1, :total, :depth], onehot)
            weight = jnp.maximum(-slopes(normals, trig, k, lo, hi), 0.0)
            for g in range(0, bands, unit):
                height = up_to(min(unit, bands - g) * angles, 8)
                window = slice(g * angles, g * angles + height)
                piece = weight[:height] * values[window]
                if k:
                    piece = piece + acc[window, lo:hi]
                acc[window, lo:hi] = piece
            for _ in range(-(-bands // index.shape[0])):
                if waiting:
                    finish(*waiting.pop(0))
        for item in waiting:
            finish(*item)
        waiting = [(f, lo, hi) for f in range(bands)]
    for item in waiting:
        finish(*item)


def local_kernel(*refs, first, unit):
    if first:
        (action, source_hbm, speeds_hbm, index, normals, nodal, trig) = refs[:7]
        part, invd, invs, base, rows, acc, source, speeds, arrived, came = refs[7:]
        copy = pltpu.make_async_copy(source_hbm, source, arrived)
        copy.start()
        fetch = pltpu.make_async_copy(speeds_hbm, speeds, came)
        fetch.start()
    else:
        (action, invd, invs, base, index, normals, nodal, trig) = refs[:8]
        part, rows, acc = refs[8:]
    bands, angles, local = action.shape
    store_groups(rows, lambda f: action[f], bands, angles, unit)
    if first:
        copy.wait()
        fetch.wait()

    def finish(f, lo, hi):
        here = action[f, :, lo:hi]
        shift = nodal[SHIFT : SHIFT + 1, lo:hi]
        turning = nodal[REFRACT : REFRACT + 1, lo:hi] * trig[0, :angles, : hi - lo]
        if first:
            outflow = jnp.zeros((angles, hi - lo), jnp.float32)
            wave = [trig[i, :angles, : hi - lo] for i in range(2)]
            weight = nodal[WEIGHT : WEIGHT + 1, lo:hi]
            if f == 0:
                for k in range(index.shape[0]):
                    outflow = outflow + jnp.maximum(slopes(normals, wave, k, lo, hi), 0.0)
                kept[lo] = (outflow, weight + jnp.abs(turning) + jnp.abs(shift))
            outflow, fixed = kept[lo]
            inv = 1.0 / (fixed + speeds[0, f] * outflow)
            start = (weight * here + source[f, :, lo:hi]) * inv
            scaled = speeds[0, f] * inv
            invd[f, :, lo:hi] = inv
            invs[f, :, lo:hi] = scaled
            base[f, :, lo:hi] = start
        else:
            inv, scaled, start = invd[f, :, lo:hi], invs[f, :, lo:hi], base[f, :, lo:hi]
        before = jnp.concatenate([here[angles - 1 :], here[: angles - 1]], axis=0)
        after = jnp.concatenate([here[1:], here[:1]], axis=0)
        inflow = jnp.maximum(turning, 0.0) * before + jnp.maximum(-turning, 0.0) * after
        if f > 0:
            inflow = inflow + jnp.maximum(shift, 0.0) * action[f - 1, :, lo:hi]
        if f < bands - 1:
            inflow = inflow + jnp.maximum(-shift, 0.0) * action[f + 1, :, lo:hi]
        edges = acc[f * angles : (f + 1) * angles, lo:hi]
        part[f, :, lo:hi] = start + inflow * inv + edges * scaled

    kept = {}
    gathered(acc, rows, index, normals, trig, 0, local, bands, angles, unit, finish)


def halo_kernel(*refs, routes, width, last, unit):
    halos, refs = refs[:routes], refs[routes:]
    (edge_a, edge_b, part, invd, invs, index, normals, nodal, trig), refs = refs[:9], refs[9:]
    if last:
        out, rows, acc = refs
    else:
        picks, out = refs[:2]
        parcels, edges, (rows, acc) = refs[2 : 2 + routes], refs[-4:-2], refs[-2:]
    bands, angles, local = part.shape
    depth = up_to(routes * width, 128)
    blocks = [halo[...] for halo in halos]
    if depth > routes * width:
        blocks.append(jnp.zeros((depth - routes * width, blocks[0].shape[1]), jnp.float32))
    high, low = split(jnp.concatenate(blocks, axis=0).T)
    rows[0, :, :depth] = high
    rows[1, :, :depth] = low
    is_even = nodal[EVEN : EVEN + 1, :] > 0.5

    def finish(f, lo, hi):
        value = part[f, :, lo:hi] + acc[f * angles : (f + 1) * angles, lo:hi] * invs[f, :, lo:hi]
        even = is_even[:, lo:hi]
        if f == 0:
            below = jnp.where(even, edge_b[:, lo:hi], edge_a[:, lo:hi])
            value = value + nodal[RISE : RISE + 1, lo:hi] * below * invd[f, :, lo:hi]
        if f == bands - 1:
            above = jnp.where(even, edge_a[:, lo:hi], edge_b[:, lo:hi])
            value = value + nodal[FALL : FALL + 1, lo:hi] * above * invd[f, :, lo:hi]
        out[f, :, lo:hi] = value

    gathered(acc, rows, index, normals, trig, local, depth, bands, angles, unit, finish)
    if not last:
        clear_tail(rows, bands * angles)
        store_groups(rows, lambda f: out[f], bands, angles, unit)
        emit(rows, picks, is_even, out, parcels, edges, width)


def body(
    action_old,
    source,
    time_weight,
    group_speed,
    normals,
    refract,
    freq_shift,
    nbr_list,
    send_nodes,
    adjacency,
):
    bands, angles, local = action_old.shape
    slots, width = send_nodes.shape[1:]
    degree = adjacency.shape[0]
    count = lax.axis_size("node")
    groups = lax.axis_size("freq")
    routes = node_routes(count)
    edge_routes = band_routes(groups)
    total = len(routes)
    unit = 8 // math.gcd(angles, 8)
    lanes = up_to(bands * angles, 128)
    depth = up_to(total * width, 128)

    theta = 2.0 * math.pi * np.arange(angles).astype(np.float32) / angles
    trig = np.stack([np.cos(theta), np.sin(theta)]).astype(np.float32)[:, :, None]
    trig = jnp.asarray(np.concatenate([trig] * unit, axis=1))

    f32, i32, bf16 = jnp.float32, jnp.int32, jnp.bfloat16
    shape = jax.ShapeDtypeStruct
    cube = shape((bands, angles, local), f32)
    outgoing = [shape((width, lanes), f32)] * total + [shape((angles, local), f32)] * 2
    tables = [
        shape((total * width, local), bf16),
        cube,
        shape((degree, local), i32),
        shape((2, degree, local), f32),
        shape((TABLE, local), f32),
        shape((2, unit * angles, TILE), f32),
    ]
    rows = pltpu.VMEM((2, lanes, max(local, depth)), bf16)
    acc = pltpu.VMEM((up_to(bands * angles, 8), local), f32)
    dma = pltpu.SemaphoreType.DMA
    vmem = pl.BlockSpec(memory_space=pltpu.VMEM)
    far = pl.BlockSpec(memory_space=pltpu.HBM)
    params = pltpu.CompilerParams(vmem_limit_bytes=24 * 2**20)

    def call(kernel, arrays, outs, scratch, depth_rows, distant=(), **options):
        flops = 4 * bands * angles * depth_rows * degree * local
        arrays = [
            pltpu.with_memory_space_constraint(x, pltpu.HBM) if i in distant else x
            for i, x in enumerate(arrays)
        ]
        return pl.pallas_call(
            functools.partial(kernel, unit=unit, **options),
            in_specs=[far if i in distant else vmem for i in range(len(arrays))],
            out_specs=[vmem] * len(outs),
            out_shape=outs,
            scratch_shapes=scratch,
            compiler_params=params,
            cost_estimate=pl.CostEstimate(
                flops=flops, transcendentals=0, bytes_accessed=4 * bands * angles * local
            ),
        )(*arrays)

    nodal = [x.reshape(1, local) for x in (time_weight, refract, freq_shift)]
    prepared = call(
        prep_kernel,
        [action_old, nbr_list, send_nodes.reshape(slots, 1, width), adjacency, normals, *nodal, trig],
        outgoing + tables,
        [
            rows,
            pltpu.SMEM((1, slots), i32),
            pltpu.VMEM((slots, 1, width), i32),
            pltpu.VMEM((degree, local), i32),
            pltpu.VMEM((2, degree, local), f32),
            pltpu.VMEM(trig.shape, f32),
            dma((bands,)),
            dma((8,)),
        ],
        0,
        distant=range(9),
        routes=routes,
        axes=("node", "freq", count, groups),
    )
    sends = prepared[: total + 2]
    picks, spectra, *shared = prepared[total + 2 :]
    for step in range(ITERS):
        received = [
            lax.ppermute(x, "node", [(p, target_of(r, p, count)) for p in range(count)])
            for x, r in zip(sends[:total], routes)
        ]
        received += [
            lax.ppermute(x, "freq", list(enumerate(r)))
            for x, r in zip(sends[total:], edge_routes)
        ]
        if step == 0:
            part, invd, invs, base = call(
                local_kernel,
                [spectra, source, group_speed.reshape(1, bands), *shared],
                [cube] * 4,
                [
                    rows,
                    acc,
                    pltpu.VMEM((bands, angles, local), f32),
                    pltpu.SMEM((1, bands), f32),
                    dma,
                    dma,
                ],
                local,
                distant=(1, 2),
                first=True,
            )
        else:
            (part,) = call(
                local_kernel,
                [spectra, invd, invs, base, *shared],
                [cube],
                [rows, acc],
                local,
                first=False,
            )
        last = step == ITERS - 1
        spectra, *sends = call(
            halo_kernel,
            [*received, part, invd, invs, *shared] + ([] if last else [picks]),
            [cube] + ([] if last else outgoing),
            [rows, acc],
            depth,
            routes=total,
            width=width,
            last=last,
        )
    return spectra


def solution(mesh):
    in_specs = (
        P("freq", None, "node"),
        P("freq", None, "node"),
        P("node"),
        P("freq"),
        P(None, None, "node"),
        P("node"),
        P("node"),
        P("node", None),
        P("node", None, None),
        P(None, "node"),
    )
    out_specs = P("freq", None, "node")
    return jax.shard_map(body, mesh=mesh, in_specs=in_specs, out_specs=out_specs, check_vma=False)
```

```python
import functools
import math

import jax
import jax.numpy as jnp
import numpy as np
from jax import lax
from jax.experimental import pallas as pl
from jax.experimental.pallas import tpu as pltpu
from jax.sharding import PartitionSpec as P

REACH = 3
ITERS = 3
TILE = 256


def up_to(value, multiple):
    return -(-value // multiple) * multiple


def node_routes(count):
    masks = {p ^ ((p + d) % count) for p in range(count) for d in range(1, REACH + 1)}
    if count & (count - 1) == 0 and len(masks) <= 2 * REACH:
        order = [m for m in (6, 7, 5, 3, 2, 1) if m in masks]
        return [("xor", m) for m in order + sorted(masks - set(order))]
    routes = []
    for d in range(REACH, 0, -1):
        step = d & -d
        if count % (2 * step) == 0 and count > 2 * d:
            routes += [("swap", d, step, 0), ("swap", d, step, 1)]
        else:
            routes += [("shift", d), ("shift", -d)]
    return routes


def target_of(route, place, count):
    if route[0] == "xor":
        return place ^ route[1]
    if route[0] == "shift":
        return (place + route[1] + count) % count
    _, d, step, side = route
    turn = 1 - 2 * (((place // step) % 2) ^ side)
    return (place + turn * d + count) % count


def source_of(route, place, count):
    if route[0] == "shift":
        return target_of(("shift", -route[1]), place, count)
    return target_of(route, place, count)


def plan_of(routes):
    if routes[:2] == [("xor", 6), ("xor", 7)] and routes[-1] == ("xor", 1):
        groups = [[0, 1]] + [[j] for j in range(2, len(routes))]
        return groups, (0, len(groups) - 1)
    return [[j] for j in range(len(routes))], None


def band_routes(count):
    first = [(p ^ 1) if (p ^ 1) < count else p for p in range(count)]
    second = [p if p == 0 else p + (1 if p % 2 else -1) for p in range(count)]
    second = [q if q < count else p for p, q in enumerate(second)]
    if count % 2 == 0:
        second[0], second[-1] = count - 1, 0
    return [first, second]


def split(values):
    high = values.astype(jnp.bfloat16)
    low = (values - high.astype(jnp.float32)).astype(jnp.bfloat16)
    return high, low


def hot(index, first, rows):
    ids = lax.broadcasted_iota(jnp.int32, (rows, index.shape[1]), 0) + first
    return jnp.where(ids == index, 1.0, 0.0).astype(jnp.bfloat16)


def dot(left, right, contract=((1,), (0,))):
    return lax.dot_general(left, right, (contract, ((), ())), preferred_element_type=jnp.float32)


def store_groups(rows, get, bands, angles, unit):
    for g in range(0, bands, unit):
        values = [get(f) for f in range(g, min(g + unit, bands))]
        block = values[0] if len(values) == 1 else jnp.concatenate(values, axis=0)
        tail = up_to(block.shape[0], 8) - block.shape[0]
        if tail:
            block = jnp.concatenate([block, jnp.zeros((tail, block.shape[1]), jnp.float32)], axis=0)
        high, low = split(block)
        window = slice(g * angles, g * angles + block.shape[0])
        rows[0, window, : block.shape[1]] = high
        rows[1, window, : block.shape[1]] = low


def emit(rows, picks, even, fields, parcels, edges):
    local = fields.shape[2]
    nt = ((1,), (1,))
    chosen = picks[...]
    out = dot(chosen, rows[0, :, :local], nt) + dot(chosen, rows[1, :, :local], nt)
    start = 0
    for parcel in parcels:
        parcel[...] = out[start : start + parcel.shape[0], :]
        start += parcel.shape[0]
    last, first = fields[fields.shape[0] - 1], fields[0]
    edges[0][...] = jnp.where(even, last, first)
    edges[1][...] = jnp.where(even, first, last)


def clear_tail(rows, used):
    start = used // 16 * 16
    rows[:, start:, :] = jnp.zeros((2, rows.shape[1] - start, rows.shape[2]), rows.dtype)


def slopes(normals, trig, k, lo, hi):
    x = normals[0, k : k + 1, lo:hi]
    y = normals[1, k : k + 1, lo:hi]
    return trig[0] * x + trig[1] * y


WEIGHT, REFRACT, SHIFT, EVEN, RISE, FALL, TABLE = 0, 1, 2, 3, 4, 5, 8


def prep_kernel(
    action, near, sends_in, adjacency_in, normals_in, weight, refract, shift, trig_in, *refs, routes, groups_out, axes, unit
):
    node, freq, count, groups = axes
    total = len(routes)
    parcels, refs = refs[:groups_out], refs[groups_out:]
    edges, refs = refs[:2], refs[2:]
    picks, fields, index_out, normals, nodal, trig = refs[:6]
    rows, neighbours, sends, adjacency, raw, line, arrived, small = refs[6:]
    bands, angles, local = fields.shape
    slots, width = sends.shape[0], sends.shape[2]
    pairs = [
        (near, neighbours),
        (sends_in, sends),
        (adjacency_in, adjacency),
        (normals_in, raw),
        (weight, nodal.at[pl.ds(WEIGHT, 1)]),
        (refract, nodal.at[pl.ds(REFRACT, 1)]),
        (shift, nodal.at[pl.ds(SHIFT, 1)]),
        (trig_in, line),
    ]
    little = [pltpu.make_async_copy(x, y, small.at[i]) for i, (x, y) in enumerate(pairs)]
    copies = [
        pltpu.make_async_copy(action.at[f], fields.at[f], arrived.at[f]) for f in range(bands)
    ]
    for copy in little[:2] + copies + little[2:]:
        copy.start()
    place, band = lax.axis_index(node), lax.axis_index(freq)
    clear_tail(rows, bands * angles)
    for copy in little[:2]:
        copy.wait()
    near_of = [neighbours[0, s] for s in range(slots)]
    table = []
    for route in routes:
        target = target_of(route, place, count)
        slot = jnp.int32(0)
        for s in range(slots):
            slot = jnp.where(near_of[s] == target, s, slot)
        table.append(sends[slot].astype(jnp.float32))
    height = up_to(total, 8)
    if height > total:
        table.append(jnp.zeros((height - total, width), jnp.float32))
    table = jnp.concatenate(table, axis=0)
    if width % 128:
        spare = jnp.zeros((height, up_to(width, 128) - width), jnp.float32)
        table = jnp.concatenate([table, spare], axis=1)
    columns = table.T.astype(jnp.int32)
    lanes = lax.broadcasted_iota(jnp.int32, (width, local), 1)
    for j in range(total):
        hits = lanes == columns[:width, j : j + 1]
        picks[j * width : (j + 1) * width, :] = jnp.where(hits, 1.0, 0.0).astype(jnp.bfloat16)

    def get(f):
        copies[f].wait()
        return fields[f]

    store_groups(rows, get, bands, angles, unit)
    is_even = jnp.full((1, local), band % 2, jnp.int32) == 0
    emit(rows, picks, is_even, fields, parcels, edges)
    for copy in little[2:]:
        copy.wait()
    entry = adjacency[...]
    index = entry
    for s in range(slots):
        route = jnp.int32(0)
        for j, r in enumerate(routes):
            route = jnp.where(near_of[s] == source_of(r, place, count), j, route)
        inside = (entry >= local + s * width) & (entry < local + (s + 1) * width)
        index = jnp.where(inside, entry + (route - s) * width, index)
    index_out[...] = index
    used = entry != lax.broadcasted_iota(jnp.int32, entry.shape, 1)
    for i in range(2):
        normals[i] = jnp.where(used, raw[i], 0.0)
        trig[i] = jnp.broadcast_to(line[i], trig.shape[1:])
    moved = nodal[SHIFT : SHIFT + 1]
    has_below = jnp.where(band > 0, 1.0, 0.0)
    has_above = jnp.where(band < groups - 1, 1.0, 0.0)
    nodal[EVEN : EVEN + 1] = jnp.where(is_even, 1.0, 0.0)
    nodal[RISE : RISE + 1] = jnp.maximum(moved, 0.0) * has_below
    nodal[FALL : FALL + 1] = jnp.maximum(-moved, 0.0) * has_above
    nodal[FALL + 1 :] = jnp.zeros((TABLE - FALL - 1, local), jnp.float32)


def gathered(acc, rows, index, normals, trig, first, depth, bands, angles, unit, finish):
    local = index.shape[1]
    total = up_to(bands * angles, 8)
    waiting = []
    for lo in range(0, local, TILE):
        hi = min(lo + TILE, local)
        for k in range(index.shape[0]):
            onehot = hot(index[k : k + 1, lo:hi], first, depth)
            values = dot(rows[0, :total, :depth], onehot) + dot(rows[1, :total, :depth], onehot)
            weight = jnp.maximum(-slopes(normals, trig, k, lo, hi), 0.0)
            for g in range(0, bands, unit):
                height = up_to(min(unit, bands - g) * angles, 8)
                window = slice(g * angles, g * angles + height)
                piece = weight[:height] * values[window]
                if k:
                    piece = piece + acc[window, lo:hi]
                acc[window, lo:hi] = piece
            for _ in range(-(-bands // index.shape[0])):
                if waiting:
                    finish(*waiting.pop(0))
        for item in waiting:
            finish(*item)
        waiting = [(f, lo, hi) for f in range(bands)]
    for item in waiting:
        finish(*item)


def local_kernel(*refs, first, unit):
    if first:
        (action, source_hbm, speeds_hbm, index, normals, nodal, trig) = refs[:7]
        part, invd, invs, base, rows, acc, source, speeds, arrived, came = refs[7:]
        copy = pltpu.make_async_copy(source_hbm, source, arrived)
        copy.start()
        fetch = pltpu.make_async_copy(speeds_hbm, speeds, came)
        fetch.start()
    else:
        (action, invd, invs, base, index, normals, nodal, trig) = refs[:8]
        part, rows, acc = refs[8:]
    bands, angles, local = action.shape
    store_groups(rows, lambda f: action[f], bands, angles, unit)

    def finish(f, lo, hi):
        if first and (f, lo) == (0, 0):
            copy.wait()
            fetch.wait()
        here = action[f, :, lo:hi]
        shift = nodal[SHIFT : SHIFT + 1, lo:hi]
        turning = nodal[REFRACT : REFRACT + 1, lo:hi] * trig[0, :angles, : hi - lo]
        if first:
            outflow = jnp.zeros((angles, hi - lo), jnp.float32)
            wave = [trig[i, :angles, : hi - lo] for i in range(2)]
            weight = nodal[WEIGHT : WEIGHT + 1, lo:hi]
            if f == 0:
                for k in range(index.shape[0]):
                    outflow = outflow + jnp.maximum(slopes(normals, wave, k, lo, hi), 0.0)
                kept[lo] = (outflow, weight + jnp.abs(turning) + jnp.abs(shift))
            outflow, fixed = kept[lo]
            inv = 1.0 / (fixed + speeds[0, f] * outflow)
            start = (weight * here + source[f, :, lo:hi]) * inv
            scaled = speeds[0, f] * inv
            invd[f, :, lo:hi] = inv
            invs[f, :, lo:hi] = scaled
            base[f, :, lo:hi] = start
        else:
            inv, scaled, start = invd[f, :, lo:hi], invs[f, :, lo:hi], base[f, :, lo:hi]
        before = jnp.concatenate([here[angles - 1 :], here[: angles - 1]], axis=0)
        after = jnp.concatenate([here[1:], here[:1]], axis=0)
        inflow = jnp.maximum(turning, 0.0) * before + jnp.maximum(-turning, 0.0) * after
        if f > 0:
            inflow = inflow + jnp.maximum(shift, 0.0) * action[f - 1, :, lo:hi]
        if f < bands - 1:
            inflow = inflow + jnp.maximum(-shift, 0.0) * action[f + 1, :, lo:hi]
        edges = acc[f * angles : (f + 1) * angles, lo:hi]
        part[f, :, lo:hi] = start + inflow * inv + edges * scaled

    kept = {}
    gathered(acc, rows, index, normals, trig, 0, local, bands, angles, unit, finish)


def halo_kernel(*refs, routes, groups, arrivals, width, last, unit):
    halos, refs = refs[:groups], refs[groups:]
    (edge_a, edge_b, part, invd, invs, index, normals, nodal, trig), refs = refs[:9], refs[9:]
    if last:
        out, rows, acc = refs
    else:
        picks, out = refs[:2]
        parcels, edges, (rows, acc) = refs[2 : 2 + groups], refs[-4:-2], refs[-2:]
    bands, angles, local = part.shape
    depth = up_to(routes * width, 128)
    blocks = [halos[g][row : row + width, :] for g, row in arrivals]
    if depth > routes * width:
        blocks.append(jnp.zeros((depth - routes * width, blocks[0].shape[1]), jnp.float32))
    high, low = split(jnp.concatenate(blocks, axis=0).T)
    rows[0, :, :depth] = high
    rows[1, :, :depth] = low
    is_even = nodal[EVEN : EVEN + 1, :] > 0.5

    def finish(f, lo, hi):
        value = part[f, :, lo:hi] + acc[f * angles : (f + 1) * angles, lo:hi] * invs[f, :, lo:hi]
        even = is_even[:, lo:hi]
        if f == 0:
            below = jnp.where(even, edge_b[:, lo:hi], edge_a[:, lo:hi])
            value = value + nodal[RISE : RISE + 1, lo:hi] * below * invd[f, :, lo:hi]
        if f == bands - 1:
            above = jnp.where(even, edge_a[:, lo:hi], edge_b[:, lo:hi])
            value = value + nodal[FALL : FALL + 1, lo:hi] * above * invd[f, :, lo:hi]
        out[f, :, lo:hi] = value

    gathered(acc, rows, index, normals, trig, local, depth, bands, angles, unit, finish)
    if not last:
        clear_tail(rows, bands * angles)
        store_groups(rows, lambda f: out[f], bands, angles, unit)
        emit(rows, picks, is_even, out, parcels, edges)


def body(
    action_old,
    source,
    time_weight,
    group_speed,
    normals,
    refract,
    freq_shift,
    nbr_list,
    send_nodes,
    adjacency,
):
    bands, angles, local = action_old.shape
    slots, width = send_nodes.shape[1:]
    degree = adjacency.shape[0]
    count = lax.axis_size("node")
    groups = lax.axis_size("freq")
    routes = node_routes(count)
    edge_routes = band_routes(groups)
    plan, relay = plan_of(routes)
    total = len(routes)
    arrivals = [(g, place * width) for g, group in enumerate(plan) for place in range(len(group))]
    if relay:
        arrivals[1] = (relay[1], width)
    unit = 8 // math.gcd(angles, 8)
    lanes = up_to(bands * angles, 128)
    depth = up_to(total * width, 128)

    theta = 2.0 * math.pi * np.arange(angles).astype(np.float32) / angles
    trig = np.stack([np.cos(theta), np.sin(theta)]).astype(np.float32)[:, :, None]
    trig = jnp.asarray(np.concatenate([trig] * unit, axis=1))

    f32, i32, bf16 = jnp.float32, jnp.int32, jnp.bfloat16
    shape = jax.ShapeDtypeStruct
    cube = shape((bands, angles, local), f32)
    outgoing = [shape((width * len(group), lanes), f32) for group in plan]
    outgoing += [shape((angles, local), f32)] * 2
    tables = [
        shape((total * width, local), bf16),
        cube,
        shape((degree, local), i32),
        shape((2, degree, local), f32),
        shape((TABLE, local), f32),
        shape((2, unit * angles, TILE), f32),
    ]
    rows = pltpu.VMEM((2, lanes, max(local, depth)), bf16)
    acc = pltpu.VMEM((up_to(bands * angles, 8), local), f32)
    dma = pltpu.SemaphoreType.DMA
    vmem = pl.BlockSpec(memory_space=pltpu.VMEM)
    far = pl.BlockSpec(memory_space=pltpu.HBM)
    params = pltpu.CompilerParams(vmem_limit_bytes=24 * 2**20)

    def call(kernel, arrays, outs, scratch, depth_rows, distant=(), **options):
        flops = 4 * bands * angles * depth_rows * degree * local
        arrays = [
            pltpu.with_memory_space_constraint(x, pltpu.HBM) if i in distant else x
            for i, x in enumerate(arrays)
        ]
        return pl.pallas_call(
            functools.partial(kernel, unit=unit, **options),
            in_specs=[far if i in distant else vmem for i in range(len(arrays))],
            out_specs=[vmem] * len(outs),
            out_shape=outs,
            scratch_shapes=scratch,
            compiler_params=params,
            cost_estimate=pl.CostEstimate(
                flops=flops, transcendentals=0, bytes_accessed=4 * bands * angles * local
            ),
        )(*arrays)

    nodal = [x.reshape(1, local) for x in (time_weight, refract, freq_shift)]
    prepared = call(
        prep_kernel,
        [action_old, nbr_list, send_nodes.reshape(slots, 1, width), adjacency, normals, *nodal, trig],
        outgoing + tables,
        [
            rows,
            pltpu.SMEM((1, slots), i32),
            pltpu.VMEM((slots, 1, width), i32),
            pltpu.VMEM((degree, local), i32),
            pltpu.VMEM((2, degree, local), f32),
            pltpu.VMEM(trig.shape, f32),
            dma((bands,)),
            dma((8,)),
        ],
        0,
        distant=range(9),
        routes=routes,
        groups_out=len(plan),
        axes=("node", "freq", count, groups),
    )
    sends = prepared[: len(outgoing)]
    picks, spectra, *shared = prepared[len(outgoing) :]

    def along(block, group):
        route = routes[plan[group][0]]
        return lax.ppermute(block, "node", [(p, target_of(route, p, count)) for p in range(count)])

    for step in range(ITERS):
        direct = [g for g in range(len(plan)) if not relay or g != relay[1]]
        arrived = {g: along(sends[g], g) for g in direct}
        across = [
            lax.ppermute(x, "freq", list(enumerate(r)))
            for x, r in zip(sends[len(plan) :], edge_routes)
        ]
        if relay:
            passed = jnp.concatenate([sends[relay[1]], arrived[relay[0]][width:]], axis=0)
            passed, spectra = lax.optimization_barrier((passed, spectra))
            arrived[relay[1]] = along(passed, relay[1])
        received = [arrived[g] for g in range(len(plan))] + across
        if step == 0:
            part, invd, invs, base = call(
                local_kernel,
                [spectra, source, group_speed.reshape(1, bands), *shared],
                [cube] * 4,
                [
                    rows,
                    acc,
                    pltpu.VMEM((bands, angles, local), f32),
                    pltpu.SMEM((1, bands), f32),
                    dma,
                    dma,
                ],
                local,
                distant=(1, 2),
                first=True,
            )
        else:
            (part,) = call(
                local_kernel,
                [spectra, invd, invs, base, *shared],
                [cube],
                [rows, acc],
                local,
                first=False,
            )
        last = step == ITERS - 1
        spectra, *sends = call(
            halo_kernel,
            [*received, part, invd, invs, *shared] + ([] if last else [picks]),
            [cube] + ([] if last else outgoing),
            [rows, acc],
            depth,
            routes=total,
            groups=len(plan),
            arrivals=arrivals,
            width=width,
            last=last,
        )
    return spectra


def solution(mesh):
    in_specs = (
        P("freq", None, "node"),
        P("freq", None, "node"),
        P("node"),
        P("freq"),
        P(None, None, "node"),
        P("node"),
        P("node"),
        P("node", None),
        P("node", None, None),
        P(None, "node"),
    )
    out_specs = P("freq", None, "node")
    return jax.shard_map(body, mesh=mesh, in_specs=in_specs, out_specs=out_specs, check_vma=False)
```

```python
import functools
import math

import jax
import jax.numpy as jnp
import numpy as np
from jax import lax
from jax.experimental import pallas as pl
from jax.experimental.pallas import tpu as pltpu
from jax.sharding import PartitionSpec as P

REACH = 3
ITERS = 3
TILE = 256


def up_to(value, multiple):
    return -(-value // multiple) * multiple


def node_routes(count):
    masks = {p ^ ((p + d) % count) for p in range(count) for d in range(1, REACH + 1)}
    if count & (count - 1) == 0 and len(masks) <= 2 * REACH:
        order = [m for m in (6, 7, 5, 3, 2, 1) if m in masks]
        return [("xor", m) for m in order + sorted(masks - set(order))]
    routes = []
    for d in range(REACH, 0, -1):
        step = d & -d
        if count % (2 * step) == 0 and count > 2 * d:
            routes += [("swap", d, step, 0), ("swap", d, step, 1)]
        else:
            routes += [("shift", d), ("shift", -d)]
    return routes


def target_of(route, place, count):
    if route[0] == "xor":
        return place ^ route[1]
    if route[0] == "shift":
        return (place + route[1] + count) % count
    _, d, step, side = route
    turn = 1 - 2 * (((place // step) % 2) ^ side)
    return (place + turn * d + count) % count


def source_of(route, place, count):
    if route[0] == "shift":
        return target_of(("shift", -route[1]), place, count)
    return target_of(route, place, count)


def plan_of(routes):
    if routes[:2] == [("xor", 6), ("xor", 7)] and routes[-1] == ("xor", 1):
        groups = [[0, 1]] + [[j] for j in range(2, len(routes))]
        return groups, (0, len(groups) - 1)
    return [[j] for j in range(len(routes))], None


def band_routes(count):
    first = [(p ^ 1) if (p ^ 1) < count else p for p in range(count)]
    second = [p if p == 0 else p + (1 if p % 2 else -1) for p in range(count)]
    second = [q if q < count else p for p, q in enumerate(second)]
    if count % 2 == 0:
        second[0], second[-1] = count - 1, 0
    return [first, second]


def split(values):
    high = values.astype(jnp.bfloat16)
    low = (values - high.astype(jnp.float32)).astype(jnp.bfloat16)
    return high, low


def hot(index, first, rows):
    step = min(rows, 256)
    shape = (step, index.shape[1])
    ids = lax.broadcasted_iota(jnp.int32, shape, 0).astype(jnp.float32).astype(jnp.bfloat16)
    blocks = []
    for start in range(0, rows, step):
        offset = (index - (first + start)).astype(jnp.float32).astype(jnp.bfloat16)
        hits = ids == jnp.broadcast_to(offset, shape)
        blocks.append(jnp.where(hits, jnp.bfloat16(1), jnp.bfloat16(0)))
    return blocks[0] if len(blocks) == 1 else jnp.concatenate(blocks, axis=0)


def dot(left, right, contract=((1,), (0,))):
    return lax.dot_general(left, right, (contract, ((), ())), preferred_element_type=jnp.float32)


def store_groups(rows, get, bands, angles, unit):
    for g in range(0, bands, unit):
        values = [get(f) for f in range(g, min(g + unit, bands))]
        block = values[0] if len(values) == 1 else jnp.concatenate(values, axis=0)
        tail = up_to(block.shape[0], 8) - block.shape[0]
        if tail:
            block = jnp.concatenate([block, jnp.zeros((tail, block.shape[1]), jnp.float32)], axis=0)
        high, low = split(block)
        window = slice(g * angles, g * angles + block.shape[0])
        rows[0, window, : block.shape[1]] = high
        rows[1, window, : block.shape[1]] = low


def emit(rows, picks, even, fields, parcels, edges):
    local = fields.shape[2]
    nt = ((1,), (1,))
    chosen = picks[...]
    out = dot(chosen, rows[0, :, :local], nt) + dot(chosen, rows[1, :, :local], nt)
    start = 0
    for parcel in parcels:
        parcel[...] = out[start : start + parcel.shape[0], :]
        start += parcel.shape[0]
    last, first = fields[fields.shape[0] - 1], fields[0]
    edges[0][...] = jnp.where(even, last, first)
    edges[1][...] = jnp.where(even, first, last)


def clear_tail(rows, used):
    start = used // 16 * 16
    rows[:, start:, :] = jnp.zeros((2, rows.shape[1] - start, rows.shape[2]), rows.dtype)


def slopes(normals, trig, k, lo, hi):
    x = normals[0, k : k + 1, lo:hi]
    y = normals[1, k : k + 1, lo:hi]
    return trig[0] * x + trig[1] * y


WEIGHT, REFRACT, SHIFT, EVEN, RISE, FALL, TABLE = 0, 1, 2, 3, 4, 5, 8


def prep_kernel(
    action, near, sends_in, adjacency_in, normals_in, weight, refract, shift, trig_in, *refs, routes, groups_out, axes, unit
):
    node, freq, count, groups = axes
    total = len(routes)
    parcels, refs = refs[:groups_out], refs[groups_out:]
    edges, refs = refs[:2], refs[2:]
    picks, fields, index_out, normals, nodal, trig = refs[:6]
    rows, neighbours, sends, adjacency, raw, line, arrived, small = refs[6:]
    bands, angles, local = fields.shape
    slots, width = sends.shape[0], sends.shape[2]
    pairs = [
        (near, neighbours),
        (sends_in, sends),
        (adjacency_in, adjacency),
        (normals_in, raw),
        (weight, nodal.at[pl.ds(WEIGHT, 1)]),
        (refract, nodal.at[pl.ds(REFRACT, 1)]),
        (shift, nodal.at[pl.ds(SHIFT, 1)]),
        (trig_in, line),
    ]
    little = [pltpu.make_async_copy(x, y, small.at[i]) for i, (x, y) in enumerate(pairs)]
    copies = [
        pltpu.make_async_copy(action.at[f], fields.at[f], arrived.at[f]) for f in range(bands)
    ]
    for copy in little[:2] + copies + little[2:]:
        copy.start()
    place, band = lax.axis_index(node), lax.axis_index(freq)
    clear_tail(rows, bands * angles)
    for copy in little[:2]:
        copy.wait()
    near_of = [neighbours[0, s] for s in range(slots)]
    table = []
    for route in routes:
        target = target_of(route, place, count)
        slot = jnp.int32(0)
        for s in range(slots):
            slot = jnp.where(near_of[s] == target, s, slot)
        table.append(sends[slot].astype(jnp.float32))
    height = up_to(total, 8)
    if height > total:
        table.append(jnp.zeros((height - total, width), jnp.float32))
    table = jnp.concatenate(table, axis=0)
    if width % 128:
        spare = jnp.zeros((height, up_to(width, 128) - width), jnp.float32)
        table = jnp.concatenate([table, spare], axis=1)
    columns = table.T.astype(jnp.int32)
    lanes = lax.broadcasted_iota(jnp.int32, (width, local), 1)
    for j in range(total):
        hits = lanes == columns[:width, j : j + 1]
        picks[j * width : (j + 1) * width, :] = jnp.where(hits, 1.0, 0.0).astype(jnp.bfloat16)

    def get(f):
        copies[f].wait()
        return fields[f]

    store_groups(rows, get, bands, angles, unit)
    is_even = jnp.full((1, local), band % 2, jnp.int32) == 0
    emit(rows, picks, is_even, fields, parcels, edges)
    for copy in little[2:]:
        copy.wait()
    entry = adjacency[...]
    index = entry
    for s in range(slots):
        route = jnp.int32(0)
        for j, r in enumerate(routes):
            route = jnp.where(near_of[s] == source_of(r, place, count), j, route)
        inside = (entry >= local + s * width) & (entry < local + (s + 1) * width)
        index = jnp.where(inside, entry + (route - s) * width, index)
    index_out[...] = index
    used = entry != lax.broadcasted_iota(jnp.int32, entry.shape, 1)
    for i in range(2):
        normals[i] = jnp.where(used, raw[i], 0.0)
        trig[i] = jnp.broadcast_to(line[i], trig.shape[1:])
    moved = nodal[SHIFT : SHIFT + 1]
    has_below = jnp.where(band > 0, 1.0, 0.0)
    has_above = jnp.where(band < groups - 1, 1.0, 0.0)
    nodal[EVEN : EVEN + 1] = jnp.where(is_even, 1.0, 0.0)
    nodal[RISE : RISE + 1] = jnp.maximum(moved, 0.0) * has_below
    nodal[FALL : FALL + 1] = jnp.maximum(-moved, 0.0) * has_above
    nodal[FALL + 1 :] = jnp.zeros((TABLE - FALL - 1, local), jnp.float32)


def gathered(acc, rows, index, normals, trig, first, depth, bands, angles, unit, finish):
    local = index.shape[1]
    total = up_to(bands * angles, 8)
    waiting = []
    for lo in range(0, local, TILE):
        hi = min(lo + TILE, local)
        for k in range(index.shape[0]):
            onehot = hot(index[k : k + 1, lo:hi], first, depth)
            values = dot(rows[0, :total, :depth], onehot) + dot(rows[1, :total, :depth], onehot)
            weight = jnp.maximum(-slopes(normals, trig, k, lo, hi), 0.0)
            for g in range(0, bands, unit):
                height = up_to(min(unit, bands - g) * angles, 8)
                window = slice(g * angles, g * angles + height)
                piece = weight[:height] * values[window]
                if k:
                    piece = piece + acc[window, lo:hi]
                acc[window, lo:hi] = piece
            for _ in range(-(-bands // index.shape[0])):
                if waiting:
                    finish(*waiting.pop(0))
        for item in waiting:
            finish(*item)
        waiting = [(f, lo, hi) for f in range(bands)]
    for item in waiting:
        finish(*item)


def local_kernel(*refs, first, unit):
    if first:
        (action, source_hbm, speeds_hbm, index, normals, nodal, trig) = refs[:7]
        part, invd, invs, base, rows, acc, source, speeds, arrived, came = refs[7:]
        copy = pltpu.make_async_copy(source_hbm, source, arrived)
        copy.start()
        fetch = pltpu.make_async_copy(speeds_hbm, speeds, came)
        fetch.start()
    else:
        (action, invd, invs, base, index, normals, nodal, trig) = refs[:8]
        part, rows, acc = refs[8:]
    bands, angles, local = action.shape
    store_groups(rows, lambda f: action[f], bands, angles, unit)

    def finish(f, lo, hi):
        if first and (f, lo) == (0, 0):
            copy.wait()
            fetch.wait()
        here = action[f, :, lo:hi]
        shift = nodal[SHIFT : SHIFT + 1, lo:hi]
        turning = nodal[REFRACT : REFRACT + 1, lo:hi] * trig[0, :angles, : hi - lo]
        if first:
            outflow = jnp.zeros((angles, hi - lo), jnp.float32)
            wave = [trig[i, :angles, : hi - lo] for i in range(2)]
            weight = nodal[WEIGHT : WEIGHT + 1, lo:hi]
            if f == 0:
                for k in range(index.shape[0]):
                    outflow = outflow + jnp.maximum(slopes(normals, wave, k, lo, hi), 0.0)
                kept[lo] = (outflow, weight + jnp.abs(turning) + jnp.abs(shift))
            outflow, fixed = kept[lo]
            inv = 1.0 / (fixed + speeds[0, f] * outflow)
            start = (weight * here + source[f, :, lo:hi]) * inv
            scaled = speeds[0, f] * inv
            invd[f, :, lo:hi] = inv
            invs[f, :, lo:hi] = scaled
            base[f, :, lo:hi] = start
        else:
            inv, scaled, start = invd[f, :, lo:hi], invs[f, :, lo:hi], base[f, :, lo:hi]
        before = jnp.concatenate([here[angles - 1 :], here[: angles - 1]], axis=0)
        after = jnp.concatenate([here[1:], here[:1]], axis=0)
        inflow = jnp.maximum(turning, 0.0) * before + jnp.maximum(-turning, 0.0) * after
        if f > 0:
            inflow = inflow + jnp.maximum(shift, 0.0) * action[f - 1, :, lo:hi]
        if f < bands - 1:
            inflow = inflow + jnp.maximum(-shift, 0.0) * action[f + 1, :, lo:hi]
        edges = acc[f * angles : (f + 1) * angles, lo:hi]
        part[f, :, lo:hi] = start + inflow * inv + edges * scaled

    kept = {}
    gathered(acc, rows, index, normals, trig, 0, local, bands, angles, unit, finish)


def halo_kernel(*refs, routes, groups, arrivals, width, last, unit):
    halos, refs = refs[:groups], refs[groups:]
    (edge_a, edge_b, part, invd, invs, index, normals, nodal, trig), refs = refs[:9], refs[9:]
    if last:
        out, rows, acc = refs
    else:
        picks, out = refs[:2]
        parcels, edges, (rows, acc) = refs[2 : 2 + groups], refs[-4:-2], refs[-2:]
    bands, angles, local = part.shape
    depth = up_to(routes * width, 128)
    blocks = [halos[g][row : row + width, :] for g, row in arrivals]
    if depth > routes * width:
        blocks.append(jnp.zeros((depth - routes * width, blocks[0].shape[1]), jnp.float32))
    high, low = split(jnp.concatenate(blocks, axis=0).T)
    rows[0, :, :depth] = high
    rows[1, :, :depth] = low
    is_even = nodal[EVEN : EVEN + 1, :] > 0.5

    def finish(f, lo, hi):
        value = part[f, :, lo:hi] + acc[f * angles : (f + 1) * angles, lo:hi] * invs[f, :, lo:hi]
        even = is_even[:, lo:hi]
        if f == 0:
            below = jnp.where(even, edge_b[:, lo:hi], edge_a[:, lo:hi])
            value = value + nodal[RISE : RISE + 1, lo:hi] * below * invd[f, :, lo:hi]
        if f == bands - 1:
            above = jnp.where(even, edge_a[:, lo:hi], edge_b[:, lo:hi])
            value = value + nodal[FALL : FALL + 1, lo:hi] * above * invd[f, :, lo:hi]
        out[f, :, lo:hi] = value

    gathered(acc, rows, index, normals, trig, local, depth, bands, angles, unit, finish)
    if not last:
        clear_tail(rows, bands * angles)
        store_groups(rows, lambda f: out[f], bands, angles, unit)
        emit(rows, picks, is_even, out, parcels, edges)


def body(
    action_old,
    source,
    time_weight,
    group_speed,
    normals,
    refract,
    freq_shift,
    nbr_list,
    send_nodes,
    adjacency,
):
    bands, angles, local = action_old.shape
    slots, width = send_nodes.shape[1:]
    degree = adjacency.shape[0]
    count = lax.axis_size("node")
    groups = lax.axis_size("freq")
    routes = node_routes(count)
    edge_routes = band_routes(groups)
    plan, relay = plan_of(routes)
    total = len(routes)
    arrivals = [(g, place * width) for g, group in enumerate(plan) for place in range(len(group))]
    if relay:
        arrivals[1] = (relay[1], width)
    unit = 8 // math.gcd(angles, 8)
    lanes = up_to(bands * angles, 128)
    depth = up_to(total * width, 128)

    theta = 2.0 * math.pi * np.arange(angles).astype(np.float32) / angles
    trig = np.stack([np.cos(theta), np.sin(theta)]).astype(np.float32)[:, :, None]
    trig = jnp.asarray(np.concatenate([trig] * unit, axis=1))

    f32, i32, bf16 = jnp.float32, jnp.int32, jnp.bfloat16
    shape = jax.ShapeDtypeStruct
    cube = shape((bands, angles, local), f32)
    outgoing = [shape((width * len(group), lanes), f32) for group in plan]
    outgoing += [shape((angles, local), f32)] * 2
    tables = [
        shape((total * width, local), bf16),
        cube,
        shape((degree, local), i32),
        shape((2, degree, local), f32),
        shape((TABLE, local), f32),
        shape((2, unit * angles, TILE), f32),
    ]
    rows = pltpu.VMEM((2, lanes, max(local, depth)), bf16)
    acc = pltpu.VMEM((up_to(bands * angles, 8), local), f32)
    dma = pltpu.SemaphoreType.DMA
    vmem = pl.BlockSpec(memory_space=pltpu.VMEM)
    far = pl.BlockSpec(memory_space=pltpu.HBM)
    params = pltpu.CompilerParams(vmem_limit_bytes=24 * 2**20)

    def call(kernel, arrays, outs, scratch, depth_rows, distant=(), **options):
        flops = 4 * bands * angles * depth_rows * degree * local
        arrays = [
            pltpu.with_memory_space_constraint(x, pltpu.HBM) if i in distant else x
            for i, x in enumerate(arrays)
        ]
        return pl.pallas_call(
            functools.partial(kernel, unit=unit, **options),
            in_specs=[far if i in distant else vmem for i in range(len(arrays))],
            out_specs=[vmem] * len(outs),
            out_shape=outs,
            scratch_shapes=scratch,
            compiler_params=params,
            cost_estimate=pl.CostEstimate(
                flops=flops, transcendentals=0, bytes_accessed=4 * bands * angles * local
            ),
        )(*arrays)

    nodal = [x.reshape(1, local) for x in (time_weight, refract, freq_shift)]
    prepared = call(
        prep_kernel,
        [action_old, nbr_list, send_nodes.reshape(slots, 1, width), adjacency, normals, *nodal, trig],
        outgoing + tables,
        [
            rows,
            pltpu.SMEM((1, slots), i32),
            pltpu.VMEM((slots, 1, width), i32),
            pltpu.VMEM((degree, local), i32),
            pltpu.VMEM((2, degree, local), f32),
            pltpu.VMEM(trig.shape, f32),
            dma((bands,)),
            dma((8,)),
        ],
        0,
        distant=range(9),
        routes=routes,
        groups_out=len(plan),
        axes=("node", "freq", count, groups),
    )
    sends = prepared[: len(outgoing)]
    picks, spectra, *shared = prepared[len(outgoing) :]

    def along(block, group):
        route = routes[plan[group][0]]
        return lax.ppermute(block, "node", [(p, target_of(route, p, count)) for p in range(count)])

    for step in range(ITERS):
        direct = [g for g in range(len(plan)) if not relay or g != relay[1]]
        arrived = {g: along(sends[g], g) for g in direct}
        across = [
            lax.ppermute(x, "freq", list(enumerate(r)))
            for x, r in zip(sends[len(plan) :], edge_routes)
        ]
        if relay:
            passed = jnp.concatenate([sends[relay[1]], arrived[relay[0]][width:]], axis=0)
            passed, spectra = lax.optimization_barrier((passed, spectra))
            arrived[relay[1]] = along(passed, relay[1])
        received = [arrived[g] for g in range(len(plan))] + across
        if step == 0:
            part, invd, invs, base = call(
                local_kernel,
                [spectra, source, group_speed.reshape(1, bands), *shared],
                [cube] * 4,
                [
                    rows,
                    acc,
                    pltpu.VMEM((bands, angles, local), f32),
                    pltpu.SMEM((1, bands), f32),
                    dma,
                    dma,
                ],
                local,
                distant=(1, 2),
                first=True,
            )
        else:
            (part,) = call(
                local_kernel,
                [spectra, invd, invs, base, *shared],
                [cube],
                [rows, acc],
                local,
                first=False,
            )
        last = step == ITERS - 1
        spectra, *sends = call(
            halo_kernel,
            [*received, part, invd, invs, *shared] + ([] if last else [picks]),
            [cube] + ([] if last else outgoing),
            [rows, acc],
            depth,
            routes=total,
            groups=len(plan),
            arrivals=arrivals,
            width=width,
            last=last,
        )
    return spectra


def solution(mesh):
    in_specs = (
        P("freq", None, "node"),
        P("freq", None, "node"),
        P("node"),
        P("freq"),
        P(None, None, "node"),
        P("node"),
        P("node"),
        P("node", None),
        P("node", None, None),
        P(None, "node"),
    )
    out_specs = P("freq", None, "node")
    return jax.shard_map(body, mesh=mesh, in_specs=in_specs, out_specs=out_specs, check_vma=False)
```

```python
import functools
import math

import jax
import jax.numpy as jnp
import numpy as np
from jax import lax
from jax.experimental import pallas as pl
from jax.experimental.pallas import tpu as pltpu
from jax.sharding import PartitionSpec as P

REACH = 3
ITERS = 3
TILE = 256


def up_to(value, multiple):
    return -(-value // multiple) * multiple


def node_routes(count):
    masks = {p ^ ((p + d) % count) for p in range(count) for d in range(1, REACH + 1)}
    if count & (count - 1) == 0 and len(masks) <= 2 * REACH:
        order = [m for m in (6, 7, 5, 3, 2, 1) if m in masks]
        return [("xor", m) for m in order + sorted(masks - set(order))]
    routes = []
    for d in range(REACH, 0, -1):
        step = d & -d
        if count % (2 * step) == 0 and count > 2 * d:
            routes += [("swap", d, step, 0), ("swap", d, step, 1)]
        else:
            routes += [("shift", d), ("shift", -d)]
    return routes


def target_of(route, place, count):
    if route[0] == "xor":
        return place ^ route[1]
    if route[0] == "shift":
        return (place + route[1] + count) % count
    _, d, step, side = route
    turn = 1 - 2 * (((place // step) % 2) ^ side)
    return (place + turn * d + count) % count


def source_of(route, place, count):
    if route[0] == "shift":
        return target_of(("shift", -route[1]), place, count)
    return target_of(route, place, count)


def plan_of(routes):
    if routes[:2] == [("xor", 6), ("xor", 7)] and routes[-1] == ("xor", 1):
        groups = [[0, 1]] + [[j] for j in range(2, len(routes))]
        return groups, (0, len(groups) - 1)
    return [[j] for j in range(len(routes))], None


def band_routes(count):
    first = [(p ^ 1) if (p ^ 1) < count else p for p in range(count)]
    second = [p if p == 0 else p + (1 if p % 2 else -1) for p in range(count)]
    second = [q if q < count else p for p, q in enumerate(second)]
    if count % 2 == 0:
        second[0], second[-1] = count - 1, 0
    return [first, second]


def split(values):
    high = values.astype(jnp.bfloat16)
    low = (values - high.astype(jnp.float32)).astype(jnp.bfloat16)
    return high, low


def hot(index, first, rows):
    step = min(rows, 256)
    shape = (step, index.shape[1])
    ids = lax.broadcasted_iota(jnp.int32, shape, 0).astype(jnp.float32).astype(jnp.bfloat16)
    blocks = []
    for start in range(0, rows, step):
        offset = (index - (first + start)).astype(jnp.float32).astype(jnp.bfloat16)
        hits = ids == jnp.broadcast_to(offset, shape)
        blocks.append(jnp.where(hits, jnp.bfloat16(1), jnp.bfloat16(0)))
    return blocks[0] if len(blocks) == 1 else jnp.concatenate(blocks, axis=0)


def dot(left, right, contract=((1,), (0,))):
    return lax.dot_general(left, right, (contract, ((), ())), preferred_element_type=jnp.float32)


def store_groups(rows, get, bands, angles, unit):
    for g in range(0, bands, unit):
        values = [get(f) for f in range(g, min(g + unit, bands))]
        block = values[0] if len(values) == 1 else jnp.concatenate(values, axis=0)
        tail = up_to(block.shape[0], 8) - block.shape[0]
        if tail:
            block = jnp.concatenate([block, jnp.zeros((tail, block.shape[1]), jnp.float32)], axis=0)
        high, low = split(block)
        window = slice(g * angles, g * angles + block.shape[0])
        rows[0, window, : block.shape[1]] = high
        rows[1, window, : block.shape[1]] = low


def emit(rows, picks, even, fields, parcels, edges):
    local = fields.shape[2]
    nt = ((1,), (1,))
    chosen = picks[...]
    out = dot(chosen, rows[0, :, :local], nt) + dot(chosen, rows[1, :, :local], nt)
    start = 0
    for parcel in parcels:
        parcel[...] = out[start : start + parcel.shape[0], :]
        start += parcel.shape[0]
    last, first = fields[fields.shape[0] - 1], fields[0]
    edges[0][...] = jnp.where(even, last, first)
    edges[1][...] = jnp.where(even, first, last)


def clear_tail(rows, used):
    start = used // 16 * 16
    rows[:, start:, :] = jnp.zeros((2, rows.shape[1] - start, rows.shape[2]), rows.dtype)


def slopes(normals, trig, k, lo, hi):
    x = normals[0, k : k + 1, lo:hi]
    y = normals[1, k : k + 1, lo:hi]
    return trig[0] * x + trig[1] * y


WEIGHT, REFRACT, SHIFT, EVEN, RISE, FALL, TABLE = 0, 1, 2, 3, 4, 5, 8


def prep_kernel(
    action,
    near,
    sends_in,
    adjacency_in,
    normals_in,
    weight,
    refract,
    shift,
    trig_in,
    *refs,
    routes,
    columns_of,
    groups_out,
    axes,
    unit,
):
    node, freq, count, groups = axes
    total = len(routes)
    parcels, refs = refs[:groups_out], refs[groups_out:]
    edges, refs = refs[:2], refs[2:]
    picks, fields, index_out, normals, nodal, trig = refs[:6]
    rows, neighbours, sends, adjacency, raw, line, arrived, small = refs[6:]
    bands, angles, local = fields.shape
    slots, width = sends.shape[0], sends.shape[2]
    pairs = [
        (near, neighbours),
        (sends_in, sends),
        (adjacency_in, adjacency),
        (normals_in, raw),
        (weight, nodal.at[pl.ds(WEIGHT, 1)]),
        (refract, nodal.at[pl.ds(REFRACT, 1)]),
        (shift, nodal.at[pl.ds(SHIFT, 1)]),
        (trig_in, line),
    ]
    little = [pltpu.make_async_copy(x, y, small.at[i]) for i, (x, y) in enumerate(pairs)]
    copies = [
        pltpu.make_async_copy(action.at[f], fields.at[f], arrived.at[f]) for f in range(bands)
    ]
    for copy in little[:2] + copies + little[2:]:
        copy.start()
    place, band = lax.axis_index(node), lax.axis_index(freq)
    clear_tail(rows, bands * angles)
    for copy in little[:2]:
        copy.wait()
    near_of = [neighbours[0, s] for s in range(slots)]
    table = []
    for route in routes:
        target = target_of(route, place, count)
        slot = jnp.int32(0)
        for s in range(slots):
            slot = jnp.where(near_of[s] == target, s, slot)
        table.append(sends[slot].astype(jnp.float32))
    height = up_to(total, 8)
    if height > total:
        table.append(jnp.zeros((height - total, width), jnp.float32))
    table = jnp.concatenate(table, axis=0)
    if width % 128:
        spare = jnp.zeros((height, up_to(width, 128) - width), jnp.float32)
        table = jnp.concatenate([table, spare], axis=1)
    columns = table.T.astype(jnp.int32)
    lanes = lax.broadcasted_iota(jnp.int32, (width, local), 1)
    for j in range(total):
        hits = lanes == columns[:width, j : j + 1]
        picks[j * width : (j + 1) * width, :] = jnp.where(hits, 1.0, 0.0).astype(jnp.bfloat16)

    def get(f):
        copies[f].wait()
        return fields[f]

    store_groups(rows, get, bands, angles, unit)
    is_even = jnp.full((1, local), band % 2, jnp.int32) == 0
    emit(rows, picks, is_even, fields, parcels, edges)
    for copy in little[2:]:
        copy.wait()
    entry = adjacency[...]
    index = entry
    for s in range(slots):
        column = jnp.int32(0)
        for r, c in zip(routes, columns_of):
            column = jnp.where(near_of[s] == source_of(r, place, count), c, column)
        inside = (entry >= local + s * width) & (entry < local + (s + 1) * width)
        index = jnp.where(inside, entry + column - s * width, index)
    index_out[...] = index
    used = entry != lax.broadcasted_iota(jnp.int32, entry.shape, 1)
    for i in range(2):
        normals[i] = jnp.where(used, raw[i], 0.0)
        trig[i] = jnp.broadcast_to(line[i], trig.shape[1:])
    moved = nodal[SHIFT : SHIFT + 1]
    has_below = jnp.where(band > 0, 1.0, 0.0)
    has_above = jnp.where(band < groups - 1, 1.0, 0.0)
    nodal[EVEN : EVEN + 1] = jnp.where(is_even, 1.0, 0.0)
    nodal[RISE : RISE + 1] = jnp.maximum(moved, 0.0) * has_below
    nodal[FALL : FALL + 1] = jnp.maximum(-moved, 0.0) * has_above
    nodal[FALL + 1 :] = jnp.zeros((TABLE - FALL - 1, local), jnp.float32)


def stack_parcels(stack, halos, arrivals, width):
    depth = stack.shape[1] // 2
    blocks = [halos[g][row : row + width, :] for g, row in arrivals]
    if depth > len(blocks) * width:
        spare = depth - len(blocks) * width
        blocks.append(jnp.zeros((spare, blocks[0].shape[1]), jnp.float32))
    high, low = split(jnp.concatenate(blocks, axis=0).T)
    stack[:, :depth] = high
    stack[:, depth:] = low


def gathered(acc, rows, stack, index, normals, trig, first, bands, angles, unit, finish):
    local = index.shape[1]
    total = up_to(bands * angles, 8)
    waiting = []
    for lo in range(0, local, TILE):
        hi = min(lo + TILE, local)
        for k in range(index.shape[0]):
            entry = index[k : k + 1, lo:hi]
            terms = []
            if rows is not None:
                onehot = hot(entry, 0, local)
                terms += [dot(rows[i, :total, :local], onehot) for i in range(2)]
            if stack is not None:
                onehot = hot(entry, first, stack.shape[1] // 2)
                terms.append(dot(stack[:total], jnp.concatenate([onehot, onehot], axis=0)))
            values = functools.reduce(jnp.add, terms)
            weight = jnp.maximum(-slopes(normals, trig, k, lo, hi), 0.0)
            for g in range(0, bands, unit):
                height = up_to(min(unit, bands - g) * angles, 8)
                window = slice(g * angles, g * angles + height)
                piece = weight[:height] * values[window]
                if k:
                    piece = piece + acc[window, lo:hi]
                acc[window, lo:hi] = piece
            for _ in range(-(-bands // index.shape[0])):
                if waiting:
                    finish(*waiting.pop(0))
        for item in waiting:
            finish(*item)
        waiting = [(f, lo, hi) for f in range(bands)]
    for item in waiting:
        finish(*item)


def local_kernel(*refs, first, arrivals, groups, width, unit):
    halos, refs = refs[:groups], refs[groups:]
    stack = None
    if arrivals:
        stack, refs = refs[-1], refs[:-1]
    if first:
        (action, source_hbm, speeds_hbm, index, normals, nodal, trig) = refs[:7]
        part, invd, invs, base, rows, acc, source, speeds, arrived, came = refs[7:]
        copy = pltpu.make_async_copy(source_hbm, source, arrived)
        copy.start()
        fetch = pltpu.make_async_copy(speeds_hbm, speeds, came)
        fetch.start()
    else:
        (action, invd, invs, base, index, normals, nodal, trig) = refs[:8]
        part, rows, acc = refs[8:]
    bands, angles, local = action.shape
    store_groups(rows, lambda f: action[f], bands, angles, unit)
    if arrivals:
        stack_parcels(stack, halos, arrivals, width)

    def finish(f, lo, hi):
        if first and (f, lo) == (0, 0):
            copy.wait()
            fetch.wait()
        here = action[f, :, lo:hi]
        shift = nodal[SHIFT : SHIFT + 1, lo:hi]
        turning = nodal[REFRACT : REFRACT + 1, lo:hi] * trig[0, :angles, : hi - lo]
        if first:
            outflow = jnp.zeros((angles, hi - lo), jnp.float32)
            wave = [trig[i, :angles, : hi - lo] for i in range(2)]
            weight = nodal[WEIGHT : WEIGHT + 1, lo:hi]
            if f == 0:
                for k in range(index.shape[0]):
                    outflow = outflow + jnp.maximum(slopes(normals, wave, k, lo, hi), 0.0)
                kept[lo] = (outflow, weight + jnp.abs(turning) + jnp.abs(shift))
            outflow, fixed = kept[lo]
            inv = 1.0 / (fixed + speeds[0, f] * outflow)
            start = (weight * here + source[f, :, lo:hi]) * inv
            scaled = speeds[0, f] * inv
            invd[f, :, lo:hi] = inv
            invs[f, :, lo:hi] = scaled
            base[f, :, lo:hi] = start
        else:
            inv, scaled, start = invd[f, :, lo:hi], invs[f, :, lo:hi], base[f, :, lo:hi]
        before = jnp.concatenate([here[angles - 1 :], here[: angles - 1]], axis=0)
        after = jnp.concatenate([here[1:], here[:1]], axis=0)
        inflow = jnp.maximum(turning, 0.0) * before + jnp.maximum(-turning, 0.0) * after
        if f > 0:
            inflow = inflow + jnp.maximum(shift, 0.0) * action[f - 1, :, lo:hi]
        if f < bands - 1:
            inflow = inflow + jnp.maximum(-shift, 0.0) * action[f + 1, :, lo:hi]
        edges = acc[f * angles : (f + 1) * angles, lo:hi]
        part[f, :, lo:hi] = start + inflow * inv + edges * scaled

    kept = {}
    gathered(acc, rows, stack, index, normals, trig, local, bands, angles, unit, finish)


def halo_kernel(*refs, groups, arrivals, first, width, last, unit):
    halos, refs = refs[:groups], refs[groups:]
    (edge_a, edge_b, part, invd, invs, index, normals, nodal, trig), refs = refs[:9], refs[9:]
    if last:
        out, acc, stack = refs
    else:
        picks, out = refs[:2]
        parcels, edges, (acc, stack, rows) = refs[2:-5], refs[-5:-3], refs[-3:]
    bands, angles, local = part.shape
    stack_parcels(stack, halos, arrivals, width)
    is_even = nodal[EVEN : EVEN + 1, :] > 0.5

    def finish(f, lo, hi):
        value = part[f, :, lo:hi] + acc[f * angles : (f + 1) * angles, lo:hi] * invs[f, :, lo:hi]
        even = is_even[:, lo:hi]
        if f == 0:
            below = jnp.where(even, edge_b[:, lo:hi], edge_a[:, lo:hi])
            value = value + nodal[RISE : RISE + 1, lo:hi] * below * invd[f, :, lo:hi]
        if f == bands - 1:
            above = jnp.where(even, edge_a[:, lo:hi], edge_b[:, lo:hi])
            value = value + nodal[FALL : FALL + 1, lo:hi] * above * invd[f, :, lo:hi]
        out[f, :, lo:hi] = value

    gathered(acc, None, stack, index, normals, trig, first, bands, angles, unit, finish)
    if not last:
        clear_tail(rows, bands * angles)
        store_groups(rows, lambda f: out[f], bands, angles, unit)
        emit(rows, picks, is_even, out, parcels, edges)


def body(
    action_old,
    source,
    time_weight,
    group_speed,
    normals,
    refract,
    freq_shift,
    nbr_list,
    send_nodes,
    adjacency,
):
    bands, angles, local = action_old.shape
    slots, width = send_nodes.shape[1:]
    degree = adjacency.shape[0]
    count = lax.axis_size("node")
    groups = lax.axis_size("freq")
    routes = node_routes(count)
    edge_routes = band_routes(groups)
    plan, relay = plan_of(routes)
    total = len(routes)
    arrivals = [(g, place * width) for g, group in enumerate(plan) for place in range(len(group))]
    if relay:
        arrivals[1] = (relay[1], width)
    early = [j for j in range(total) if relay and arrivals[j][0] != relay[1]]
    late = [j for j in range(total) if j not in early]
    margin = up_to(len(early) * width, 128)
    columns_of = [
        early.index(j) * width if j in early else margin + late.index(j) * width
        for j in range(total)
    ]
    unit = 8 // math.gcd(angles, 8)
    lanes = up_to(bands * angles, 128)

    theta = 2.0 * math.pi * np.arange(angles).astype(np.float32) / angles
    trig = np.stack([np.cos(theta), np.sin(theta)]).astype(np.float32)[:, :, None]
    trig = jnp.asarray(np.concatenate([trig] * unit, axis=1))

    f32, i32, bf16 = jnp.float32, jnp.int32, jnp.bfloat16
    shape = jax.ShapeDtypeStruct
    cube = shape((bands, angles, local), f32)
    outgoing = [shape((width * len(group), lanes), f32) for group in plan]
    outgoing += [shape((angles, local), f32)] * 2
    tables = [
        shape((total * width, local), bf16),
        cube,
        shape((degree, local), i32),
        shape((2, degree, local), f32),
        shape((TABLE, local), f32),
        shape((2, unit * angles, TILE), f32),
    ]
    rows = pltpu.VMEM((2, lanes, local), bf16)

    def stack(members):
        return pltpu.VMEM((lanes, 2 * up_to(len(members) * width, 128)), bf16)

    def places(members):
        used = sorted({arrivals[j][0] for j in members})
        return used, [(used.index(arrivals[j][0]), arrivals[j][1]) for j in members]

    early_groups, early_arrivals = places(early)
    late_groups, late_arrivals = places(late)
    acc = pltpu.VMEM((up_to(bands * angles, 8), local), f32)
    dma = pltpu.SemaphoreType.DMA
    vmem = pl.BlockSpec(memory_space=pltpu.VMEM)
    far = pl.BlockSpec(memory_space=pltpu.HBM)
    params = pltpu.CompilerParams(vmem_limit_bytes=24 * 2**20)

    def call(kernel, arrays, outs, scratch, depth_rows, distant=(), **options):
        flops = 4 * bands * angles * depth_rows * degree * local
        arrays = [
            pltpu.with_memory_space_constraint(x, pltpu.HBM) if i in distant else x
            for i, x in enumerate(arrays)
        ]
        return pl.pallas_call(
            functools.partial(kernel, unit=unit, **options),
            in_specs=[far if i in distant else vmem for i in range(len(arrays))],
            out_specs=[vmem] * len(outs),
            out_shape=outs,
            scratch_shapes=scratch,
            compiler_params=params,
            cost_estimate=pl.CostEstimate(
                flops=flops, transcendentals=0, bytes_accessed=4 * bands * angles * local
            ),
        )(*arrays)

    nodal = [x.reshape(1, local) for x in (time_weight, refract, freq_shift)]
    prepared = call(
        prep_kernel,
        [action_old, nbr_list, send_nodes.reshape(slots, 1, width), adjacency, normals, *nodal, trig],
        outgoing + tables,
        [
            rows,
            pltpu.SMEM((1, slots), i32),
            pltpu.VMEM((slots, 1, width), i32),
            pltpu.VMEM((degree, local), i32),
            pltpu.VMEM((2, degree, local), f32),
            pltpu.VMEM(trig.shape, f32),
            dma((bands,)),
            dma((8,)),
        ],
        0,
        distant=range(9),
        routes=routes,
        columns_of=columns_of,
        groups_out=len(plan),
        axes=("node", "freq", count, groups),
    )
    sends = prepared[: len(outgoing)]
    picks, spectra, *shared = prepared[len(outgoing) :]

    def along(block, group):
        route = routes[plan[group][0]]
        return lax.ppermute(block, "node", [(p, target_of(route, p, count)) for p in range(count)])

    for step in range(ITERS):
        direct = [g for g in range(len(plan)) if not relay or g != relay[1]]
        arrived = {g: along(sends[g], g) for g in direct}
        across = [
            lax.ppermute(x, "freq", list(enumerate(r)))
            for x, r in zip(sends[len(plan) :], edge_routes)
        ]
        if relay:
            passed = jnp.concatenate([sends[relay[1]], arrived[relay[0]][width:]], axis=0)
            passed, spectra = lax.optimization_barrier((passed, spectra))
            arrived[relay[1]] = along(passed, relay[1])
        ahead = [arrived[g] for g in early_groups]
        after = [arrived[g] for g in late_groups] + across
        window = dict(arrivals=early_arrivals, groups=len(early_groups), width=width)
        stacks = [stack(early)] if early else []
        depth = local + margin // 2
        if step == 0:
            part, invd, invs, base = call(
                local_kernel,
                [*ahead, spectra, source, group_speed.reshape(1, bands), *shared],
                [cube] * 4,
                [
                    rows,
                    acc,
                    pltpu.VMEM((bands, angles, local), f32),
                    pltpu.SMEM((1, bands), f32),
                    dma,
                    dma,
                    *stacks,
                ],
                depth,
                distant=(len(ahead) + 1, len(ahead) + 2),
                first=True,
                **window,
            )
        else:
            (part,) = call(
                local_kernel,
                [*ahead, spectra, invd, invs, base, *shared],
                [cube],
                [rows, acc, *stacks],
                depth,
                first=False,
                **window,
            )
        last = step == ITERS - 1
        spectra, *sends = call(
            halo_kernel,
            [*after, part, invd, invs, *shared] + ([] if last else [picks]),
            [cube] + ([] if last else outgoing),
            [acc, stack(late)] + ([] if last else [rows]),
            up_to(len(late) * width, 128),
            groups=len(late_groups),
            arrivals=late_arrivals,
            first=local + margin,
            width=width,
            last=last,
        )
    return spectra


def solution(mesh):
    in_specs = (
        P("freq", None, "node"),
        P("freq", None, "node"),
        P("node"),
        P("freq"),
        P(None, None, "node"),
        P("node"),
        P("node"),
        P("node", None),
        P("node", None, None),
        P(None, "node"),
    )
    out_specs = P("freq", None, "node")
    return jax.shard_map(body, mesh=mesh, in_specs=in_specs, out_specs=out_specs, check_vma=False)
```

```python
import functools
import math

import jax
import jax.numpy as jnp
import numpy as np
from jax import lax
from jax.experimental import pallas as pl
from jax.experimental.pallas import tpu as pltpu
from jax.sharding import PartitionSpec as P

REACH = 3
ITERS = 3
TILE = 256


def up_to(value, multiple):
    return -(-value // multiple) * multiple


def node_routes(count):
    masks = {p ^ ((p + d) % count) for p in range(count) for d in range(1, REACH + 1)}
    if count & (count - 1) == 0 and len(masks) <= 2 * REACH:
        order = [m for m in (6, 7, 3, 2, 5, 1) if m in masks]
        return [("xor", m) for m in order + sorted(masks - set(order))]
    routes = []
    for d in range(REACH, 0, -1):
        step = d & -d
        if count % (2 * step) == 0 and count > 2 * d:
            routes += [("swap", d, step, 0), ("swap", d, step, 1)]
        else:
            routes += [("shift", d), ("shift", -d)]
    return routes


def target_of(route, place, count):
    if route[0] == "xor":
        return place ^ route[1]
    if route[0] == "shift":
        return (place + route[1] + count) % count
    _, d, step, side = route
    turn = 1 - 2 * (((place // step) % 2) ^ side)
    return (place + turn * d + count) % count


def source_of(route, place, count):
    if route[0] == "shift":
        return target_of(("shift", -route[1]), place, count)
    return target_of(route, place, count)


def plan_of(routes):
    if routes[:2] == [("xor", 6), ("xor", 7)] and routes[-1] == ("xor", 1):
        groups = [[0, 1]] + [[j] for j in range(2, len(routes))]
        return groups, (0, len(groups) - 1)
    return [[j] for j in range(len(routes))], None


def band_routes(count):
    first = [(p ^ 1) if (p ^ 1) < count else p for p in range(count)]
    second = [p if p == 0 else p + (1 if p % 2 else -1) for p in range(count)]
    second = [q if q < count else p for p, q in enumerate(second)]
    if count % 2 == 0:
        second[0], second[-1] = count - 1, 0
    return [first, second]


def split(values):
    high = values.astype(jnp.bfloat16)
    low = (values - high.astype(jnp.float32)).astype(jnp.bfloat16)
    return high, low


def hot(index, first, rows):
    step = min(rows, 256)
    shape = (step, index.shape[1])
    ids = lax.broadcasted_iota(jnp.int32, shape, 0).astype(jnp.float32).astype(jnp.bfloat16)
    blocks = []
    for start in range(0, rows, step):
        offset = (index - (first + start)).astype(jnp.float32).astype(jnp.bfloat16)
        hits = ids == jnp.broadcast_to(offset, shape)
        blocks.append(jnp.where(hits, jnp.bfloat16(1), jnp.bfloat16(0)))
    return blocks[0] if len(blocks) == 1 else jnp.concatenate(blocks, axis=0)


def dot(left, right, contract=((1,), (0,))):
    return lax.dot_general(left, right, (contract, ((), ())), preferred_element_type=jnp.float32)


def store_groups(rows, get, bands, angles, unit):
    for g in range(0, bands, unit):
        values = [get(f) for f in range(g, min(g + unit, bands))]
        block = values[0] if len(values) == 1 else jnp.concatenate(values, axis=0)
        tail = up_to(block.shape[0], 8) - block.shape[0]
        if tail:
            block = jnp.concatenate([block, jnp.zeros((tail, block.shape[1]), jnp.float32)], axis=0)
        high, low = split(block)
        window = slice(g * angles, g * angles + block.shape[0])
        rows[0, window, : block.shape[1]] = high
        rows[1, window, : block.shape[1]] = low


def emit(rows, picks, even, fields, parcels, edges):
    local = fields.shape[2]
    nt = ((1,), (1,))
    chosen = picks[...]
    out = dot(chosen, rows[0, :, :local], nt) + dot(chosen, rows[1, :, :local], nt)
    start = 0
    for parcel in parcels:
        parcel[...] = out[start : start + parcel.shape[0], :]
        start += parcel.shape[0]
    last, first = fields[fields.shape[0] - 1], fields[0]
    edges[0][...] = jnp.where(even, last, first)
    edges[1][...] = jnp.where(even, first, last)


def clear_tail(rows, used):
    start = used // 16 * 16
    rows[:, start:, :] = jnp.zeros((2, rows.shape[1] - start, rows.shape[2]), rows.dtype)


def slopes(normals, trig, k, lo, hi):
    x = normals[0, k : k + 1, lo:hi]
    y = normals[1, k : k + 1, lo:hi]
    return trig[0] * x + trig[1] * y


WEIGHT, REFRACT, SHIFT, EVEN, RISE, FALL, TABLE = 0, 1, 2, 3, 4, 5, 8


def prep_kernel(
    action,
    near,
    sends_in,
    adjacency_in,
    normals_in,
    weight,
    refract,
    shift,
    trig_in,
    *refs,
    routes,
    columns_of,
    groups_out,
    axes,
    unit,
):
    node, freq, count, groups = axes
    total = len(routes)
    parcels, refs = refs[:groups_out], refs[groups_out:]
    edges, refs = refs[:2], refs[2:]
    picks, fields, index_out, normals, nodal, trig = refs[:6]
    rows, neighbours, sends, adjacency, raw, line, arrived, small = refs[6:]
    bands, angles, local = fields.shape
    slots, width = sends.shape[0], sends.shape[2]
    pairs = [
        (near, neighbours),
        (sends_in, sends),
        (adjacency_in, adjacency),
        (normals_in, raw),
        (weight, nodal.at[pl.ds(WEIGHT, 1)]),
        (refract, nodal.at[pl.ds(REFRACT, 1)]),
        (shift, nodal.at[pl.ds(SHIFT, 1)]),
        (trig_in, line),
    ]
    little = [pltpu.make_async_copy(x, y, small.at[i]) for i, (x, y) in enumerate(pairs)]
    copies = [
        pltpu.make_async_copy(action.at[f], fields.at[f], arrived.at[f]) for f in range(bands)
    ]
    for copy in little[:2] + copies + little[2:]:
        copy.start()
    place, band = lax.axis_index(node), lax.axis_index(freq)
    clear_tail(rows, bands * angles)
    for copy in little[:2]:
        copy.wait()
    near_of = [neighbours[0, s] for s in range(slots)]
    table = []
    for route in routes:
        target = target_of(route, place, count)
        slot = jnp.int32(0)
        for s in range(slots):
            slot = jnp.where(near_of[s] == target, s, slot)
        table.append(sends[slot].astype(jnp.float32))
    height = up_to(total, 8)
    if height > total:
        table.append(jnp.zeros((height - total, width), jnp.float32))
    table = jnp.concatenate(table, axis=0)
    if width % 128:
        spare = jnp.zeros((height, up_to(width, 128) - width), jnp.float32)
        table = jnp.concatenate([table, spare], axis=1)
    columns = table.T.astype(jnp.int32)
    lanes = lax.broadcasted_iota(jnp.int32, (width, local), 1)
    for j in range(total):
        hits = lanes == columns[:width, j : j + 1]
        picks[j * width : (j + 1) * width, :] = jnp.where(hits, 1.0, 0.0).astype(jnp.bfloat16)

    def get(f):
        copies[f].wait()
        return fields[f]

    store_groups(rows, get, bands, angles, unit)
    is_even = jnp.full((1, local), band % 2, jnp.int32) == 0
    emit(rows, picks, is_even, fields, parcels, edges)
    for copy in little[2:]:
        copy.wait()
    entry = adjacency[...]
    index = entry
    for s in range(slots):
        column = jnp.int32(0)
        for r, c in zip(routes, columns_of):
            column = jnp.where(near_of[s] == source_of(r, place, count), c, column)
        inside = (entry >= local + s * width) & (entry < local + (s + 1) * width)
        index = jnp.where(inside, entry + column - s * width, index)
    index_out[...] = index
    used = entry != lax.broadcasted_iota(jnp.int32, entry.shape, 1)
    for i in range(2):
        normals[i] = jnp.where(used, raw[i], 0.0)
        trig[i] = jnp.broadcast_to(line[i], trig.shape[1:])
    moved = nodal[SHIFT : SHIFT + 1]
    has_below = jnp.where(band > 0, 1.0, 0.0)
    has_above = jnp.where(band < groups - 1, 1.0, 0.0)
    nodal[EVEN : EVEN + 1] = jnp.where(is_even, 1.0, 0.0)
    nodal[RISE : RISE + 1] = jnp.maximum(moved, 0.0) * has_below
    nodal[FALL : FALL + 1] = jnp.maximum(-moved, 0.0) * has_above
    nodal[FALL + 1 :] = jnp.zeros((TABLE - FALL - 1, local), jnp.float32)


def stack_parcels(stack, halos, arrivals, width):
    depth = stack.shape[1] // 2
    blocks = [halos[g][row : row + width, :] for g, row in arrivals]
    if depth > len(blocks) * width:
        spare = depth - len(blocks) * width
        blocks.append(jnp.zeros((spare, blocks[0].shape[1]), jnp.float32))
    high, low = split(jnp.concatenate(blocks, axis=0).T)
    stack[:, :depth] = high
    stack[:, depth:] = low


def gathered(acc, rows, stack, index, normals, trig, first, bands, angles, unit, finish):
    local = index.shape[1]
    total = up_to(bands * angles, 8)
    waiting = []
    for lo in range(0, local, TILE):
        hi = min(lo + TILE, local)
        for k in range(index.shape[0]):
            entry = index[k : k + 1, lo:hi]
            terms = []
            if rows is not None:
                onehot = hot(entry, 0, local)
                terms += [dot(rows[i, :total, :local], onehot) for i in range(2)]
            if stack is not None:
                onehot = hot(entry, first, stack.shape[1] // 2)
                terms.append(dot(stack[:total], jnp.concatenate([onehot, onehot], axis=0)))
            values = functools.reduce(jnp.add, terms)
            weight = jnp.maximum(-slopes(normals, trig, k, lo, hi), 0.0)
            for g in range(0, bands, unit):
                height = up_to(min(unit, bands - g) * angles, 8)
                window = slice(g * angles, g * angles + height)
                piece = weight[:height] * values[window]
                if k:
                    piece = piece + acc[window, lo:hi]
                acc[window, lo:hi] = piece
            for _ in range(-(-bands // index.shape[0])):
                if waiting:
                    finish(*waiting.pop(0))
        for item in waiting:
            finish(*item)
        waiting = [(f, lo, hi) for f in range(bands)]
    for item in waiting:
        finish(*item)


def local_kernel(*refs, first, arrivals, groups, width, unit):
    halos, refs = refs[:groups], refs[groups:]
    stack = None
    if arrivals:
        stack, refs = refs[-1], refs[:-1]
    if first:
        (action, source_hbm, speeds_hbm, index, normals, nodal, trig) = refs[:7]
        part, invd, invs, base, rows, acc, source, speeds, arrived, came = refs[7:]
        copy = pltpu.make_async_copy(source_hbm, source, arrived)
        copy.start()
        fetch = pltpu.make_async_copy(speeds_hbm, speeds, came)
        fetch.start()
    else:
        (action, invd, invs, base, index, normals, nodal, trig) = refs[:8]
        part, rows, acc = refs[8:]
    bands, angles, local = action.shape
    store_groups(rows, lambda f: action[f], bands, angles, unit)
    if arrivals:
        stack_parcels(stack, halos, arrivals, width)

    def finish(f, lo, hi):
        if first and (f, lo) == (0, 0):
            copy.wait()
            fetch.wait()
        here = action[f, :, lo:hi]
        shift = nodal[SHIFT : SHIFT + 1, lo:hi]
        turning = nodal[REFRACT : REFRACT + 1, lo:hi] * trig[0, :angles, : hi - lo]
        if first:
            outflow = jnp.zeros((angles, hi - lo), jnp.float32)
            wave = [trig[i, :angles, : hi - lo] for i in range(2)]
            weight = nodal[WEIGHT : WEIGHT + 1, lo:hi]
            if f == 0:
                for k in range(index.shape[0]):
                    outflow = outflow + jnp.maximum(slopes(normals, wave, k, lo, hi), 0.0)
                kept[lo] = (outflow, weight + jnp.abs(turning) + jnp.abs(shift))
            outflow, fixed = kept[lo]
            inv = 1.0 / (fixed + speeds[0, f] * outflow)
            start = (weight * here + source[f, :, lo:hi]) * inv
            scaled = speeds[0, f] * inv
            invd[f, :, lo:hi] = inv
            invs[f, :, lo:hi] = scaled
            base[f, :, lo:hi] = start
        else:
            inv, scaled, start = invd[f, :, lo:hi], invs[f, :, lo:hi], base[f, :, lo:hi]
        before = jnp.concatenate([here[angles - 1 :], here[: angles - 1]], axis=0)
        after = jnp.concatenate([here[1:], here[:1]], axis=0)
        inflow = jnp.maximum(turning, 0.0) * before + jnp.maximum(-turning, 0.0) * after
        if f > 0:
            inflow = inflow + jnp.maximum(shift, 0.0) * action[f - 1, :, lo:hi]
        if f < bands - 1:
            inflow = inflow + jnp.maximum(-shift, 0.0) * action[f + 1, :, lo:hi]
        edges = acc[f * angles : (f + 1) * angles, lo:hi]
        part[f, :, lo:hi] = start + inflow * inv + edges * scaled

    kept = {}
    gathered(acc, rows, stack, index, normals, trig, local, bands, angles, unit, finish)


def halo_kernel(*refs, groups, arrivals, first, width, last, unit):
    halos, refs = refs[:groups], refs[groups:]
    (edge_a, edge_b, part, invd, invs, index, normals, nodal, trig), refs = refs[:9], refs[9:]
    if last:
        out, acc, stack = refs
    else:
        picks, out = refs[:2]
        parcels, edges, (acc, stack, rows) = refs[2:-5], refs[-5:-3], refs[-3:]
    bands, angles, local = part.shape
    stack_parcels(stack, halos, arrivals, width)
    is_even = nodal[EVEN : EVEN + 1, :] > 0.5

    def finish(f, lo, hi):
        value = part[f, :, lo:hi] + acc[f * angles : (f + 1) * angles, lo:hi] * invs[f, :, lo:hi]
        even = is_even[:, lo:hi]
        if f == 0:
            below = jnp.where(even, edge_b[:, lo:hi], edge_a[:, lo:hi])
            value = value + nodal[RISE : RISE + 1, lo:hi] * below * invd[f, :, lo:hi]
        if f == bands - 1:
            above = jnp.where(even, edge_a[:, lo:hi], edge_b[:, lo:hi])
            value = value + nodal[FALL : FALL + 1, lo:hi] * above * invd[f, :, lo:hi]
        out[f, :, lo:hi] = value

    gathered(acc, None, stack, index, normals, trig, first, bands, angles, unit, finish)
    if not last:
        clear_tail(rows, bands * angles)
        store_groups(rows, lambda f: out[f], bands, angles, unit)
        emit(rows, picks, is_even, out, parcels, edges)


def body(
    action_old,
    source,
    time_weight,
    group_speed,
    normals,
    refract,
    freq_shift,
    nbr_list,
    send_nodes,
    adjacency,
):
    bands, angles, local = action_old.shape
    slots, width = send_nodes.shape[1:]
    degree = adjacency.shape[0]
    count = lax.axis_size("node")
    groups = lax.axis_size("freq")
    routes = node_routes(count)
    edge_routes = band_routes(groups)
    plan, relay = plan_of(routes)
    total = len(routes)
    arrivals = [(g, place * width) for g, group in enumerate(plan) for place in range(len(group))]
    if relay:
        arrivals[1] = (relay[1], width)
    early = [
        j
        for j in range(total)
        if relay and arrivals[j][0] != relay[1] and routes[j] != ("xor", 5)
    ]
    late = [j for j in range(total) if j not in early]
    margin = up_to(len(early) * width, 128)
    columns_of = [
        early.index(j) * width if j in early else margin + late.index(j) * width
        for j in range(total)
    ]
    unit = 8 // math.gcd(angles, 8)
    lanes = up_to(bands * angles, 128)

    theta = 2.0 * math.pi * np.arange(angles).astype(np.float32) / angles
    trig = np.stack([np.cos(theta), np.sin(theta)]).astype(np.float32)[:, :, None]
    trig = jnp.asarray(np.concatenate([trig] * unit, axis=1))

    f32, i32, bf16 = jnp.float32, jnp.int32, jnp.bfloat16
    shape = jax.ShapeDtypeStruct
    cube = shape((bands, angles, local), f32)
    outgoing = [shape((width * len(group), lanes), f32) for group in plan]
    outgoing += [shape((angles, local), f32)] * 2
    tables = [
        shape((total * width, local), bf16),
        cube,
        shape((degree, local), i32),
        shape((2, degree, local), f32),
        shape((TABLE, local), f32),
        shape((2, unit * angles, TILE), f32),
    ]
    rows = pltpu.VMEM((2, lanes, local), bf16)

    def stack(members):
        return pltpu.VMEM((lanes, 2 * up_to(len(members) * width, 128)), bf16)

    def places(members):
        used = sorted({arrivals[j][0] for j in members})
        return used, [(used.index(arrivals[j][0]), arrivals[j][1]) for j in members]

    early_groups, early_arrivals = places(early)
    late_groups, late_arrivals = places(late)
    acc = pltpu.VMEM((up_to(bands * angles, 8), local), f32)
    dma = pltpu.SemaphoreType.DMA
    vmem = pl.BlockSpec(memory_space=pltpu.VMEM)
    far = pl.BlockSpec(memory_space=pltpu.HBM)
    params = pltpu.CompilerParams(vmem_limit_bytes=24 * 2**20)

    def call(kernel, arrays, outs, scratch, depth_rows, distant=(), **options):
        flops = 4 * bands * angles * depth_rows * degree * local
        arrays = [
            pltpu.with_memory_space_constraint(x, pltpu.HBM) if i in distant else x
            for i, x in enumerate(arrays)
        ]
        return pl.pallas_call(
            functools.partial(kernel, unit=unit, **options),
            in_specs=[far if i in distant else vmem for i in range(len(arrays))],
            out_specs=[vmem] * len(outs),
            out_shape=outs,
            scratch_shapes=scratch,
            compiler_params=params,
            cost_estimate=pl.CostEstimate(
                flops=flops, transcendentals=0, bytes_accessed=4 * bands * angles * local
            ),
        )(*arrays)

    nodal = [x.reshape(1, local) for x in (time_weight, refract, freq_shift)]
    prepared = call(
        prep_kernel,
        [action_old, nbr_list, send_nodes.reshape(slots, 1, width), adjacency, normals, *nodal, trig],
        outgoing + tables,
        [
            rows,
            pltpu.SMEM((1, slots), i32),
            pltpu.VMEM((slots, 1, width), i32),
            pltpu.VMEM((degree, local), i32),
            pltpu.VMEM((2, degree, local), f32),
            pltpu.VMEM(trig.shape, f32),
            dma((bands,)),
            dma((8,)),
        ],
        0,
        distant=range(9),
        routes=routes,
        columns_of=columns_of,
        groups_out=len(plan),
        axes=("node", "freq", count, groups),
    )
    sends = prepared[: len(outgoing)]
    picks, spectra, *shared = prepared[len(outgoing) :]

    def along(block, group):
        route = routes[plan[group][0]]
        return lax.ppermute(block, "node", [(p, target_of(route, p, count)) for p in range(count)])

    for step in range(ITERS):
        direct = [g for g in range(len(plan)) if not relay or g != relay[1]]
        arrived = {g: along(sends[g], g) for g in direct}
        across = [
            lax.ppermute(x, "freq", list(enumerate(r)))
            for x, r in zip(sends[len(plan) :], edge_routes)
        ]
        if relay:
            passed = jnp.concatenate([sends[relay[1]], arrived[relay[0]][width:]], axis=0)
            passed, spectra = lax.optimization_barrier((passed, spectra))
            arrived[relay[1]] = along(passed, relay[1])
        ahead = [arrived[g] for g in early_groups]
        after = [arrived[g] for g in late_groups] + across
        window = dict(arrivals=early_arrivals, groups=len(early_groups), width=width)
        stacks = [stack(early)] if early else []
        depth = local + margin // 2
        if step == 0:
            part, invd, invs, base = call(
                local_kernel,
                [*ahead, spectra, source, group_speed.reshape(1, bands), *shared],
                [cube] * 4,
                [
                    rows,
                    acc,
                    pltpu.VMEM((bands, angles, local), f32),
                    pltpu.SMEM((1, bands), f32),
                    dma,
                    dma,
                    *stacks,
                ],
                depth,
                distant=(len(ahead) + 1, len(ahead) + 2),
                first=True,
                **window,
            )
        else:
            (part,) = call(
                local_kernel,
                [*ahead, spectra, invd, invs, base, *shared],
                [cube],
                [rows, acc, *stacks],
                depth,
                first=False,
                **window,
            )
        last = step == ITERS - 1
        spectra, *sends = call(
            halo_kernel,
            [*after, part, invd, invs, *shared] + ([] if last else [picks]),
            [cube] + ([] if last else outgoing),
            [acc, stack(late)] + ([] if last else [rows]),
            up_to(len(late) * width, 128),
            groups=len(late_groups),
            arrivals=late_arrivals,
            first=local + margin,
            width=width,
            last=last,
        )
    return spectra


def solution(mesh):
    in_specs = (
        P("freq", None, "node"),
        P("freq", None, "node"),
        P("node"),
        P("freq"),
        P(None, None, "node"),
        P("node"),
        P("node"),
        P("node", None),
        P("node", None, None),
        P(None, "node"),
    )
    out_specs = P("freq", None, "node")
    return jax.shard_map(body, mesh=mesh, in_specs=in_specs, out_specs=out_specs, check_vma=False)
```

```python
import functools
import math

import jax
import jax.numpy as jnp
import numpy as np
from jax import lax
from jax.experimental import pallas as pl
from jax.experimental.pallas import tpu as pltpu
from jax.sharding import PartitionSpec as P


REACH = 3
ITERS = 3
TILE = 256


def up_to(value, multiple):
    return -(-value // multiple) * multiple


def node_routes(count):
    masks = {p ^ ((p + d) % count) for p in range(count) for d in range(1, REACH + 1)}
    if count & (count - 1) == 0 and len(masks) <= 2 * REACH:
        order = [m for m in (6, 7, 2, 3, 5, 1) if m in masks]
        return [("xor", m) for m in order + sorted(masks - set(order))]
    routes = []
    for d in range(REACH, 0, -1):
        step = d & -d
        if count % (2 * step) == 0 and count > 2 * d:
            routes += [("swap", d, step, 0), ("swap", d, step, 1)]
        else:
            routes += [("shift", d), ("shift", -d)]
    return routes


def target_of(route, place, count):
    if route[0] == "xor":
        return place ^ route[1]
    if route[0] == "shift":
        return (place + route[1] + count) % count
    _, d, step, side = route
    turn = 1 - 2 * (((place // step) % 2) ^ side)
    return (place + turn * d + count) % count


def source_of(route, place, count):
    if route[0] == "shift":
        return target_of(("shift", -route[1]), place, count)
    return target_of(route, place, count)


def plan_of(routes):
    if routes[:2] == [("xor", 6), ("xor", 7)] and routes[-1] == ("xor", 1):
        groups = [[0, 1]] + [[j] for j in range(2, len(routes))]
        return groups, (0, len(groups) - 1)
    return [[j] for j in range(len(routes))], None


def band_routes(count):
    first = [(p ^ 1) if (p ^ 1) < count else p for p in range(count)]
    second = [p if p == 0 else p + (1 if p % 2 else -1) for p in range(count)]
    second = [q if q < count else p for p, q in enumerate(second)]
    if count % 2 == 0:
        second[0], second[-1] = count - 1, 0
    return [first, second]


def split(values):
    high = values.astype(jnp.bfloat16)
    low = (values - high.astype(jnp.float32)).astype(jnp.bfloat16)
    return high, low


def hot(index, first, rows):
    step = min(rows, 256)
    shape = (step, index.shape[1])
    ids = lax.broadcasted_iota(jnp.int32, shape, 0).astype(jnp.float32).astype(jnp.bfloat16)
    blocks = []
    for start in range(0, rows, step):
        offset = (index - (first + start)).astype(jnp.float32).astype(jnp.bfloat16)
        hits = ids == jnp.broadcast_to(offset, shape)
        blocks.append(jnp.where(hits, jnp.bfloat16(1), jnp.bfloat16(0)))
    return blocks[0] if len(blocks) == 1 else jnp.concatenate(blocks, axis=0)


def dot(left, right, contract=((1,), (0,))):
    return lax.dot_general(left, right, (contract, ((), ())), preferred_element_type=jnp.float32)


def store_groups(rows, get, bands, angles, unit):
    for g in range(0, bands, unit):
        values = [get(f) for f in range(g, min(g + unit, bands))]
        block = values[0] if len(values) == 1 else jnp.concatenate(values, axis=0)
        tail = up_to(block.shape[0], 8) - block.shape[0]
        if tail:
            block = jnp.concatenate([block, jnp.zeros((tail, block.shape[1]), jnp.float32)], axis=0)
        high, low = split(block)
        window = slice(g * angles, g * angles + block.shape[0])
        rows[0, window, : block.shape[1]] = high
        rows[1, window, : block.shape[1]] = low


def emit(rows, picks, even, fields, parcels, edges):
    local = fields.shape[2]
    nt = ((1,), (1,))
    chosen = picks[...]
    out = dot(chosen, rows[0, :, :local], nt) + dot(chosen, rows[1, :, :local], nt)
    start = 0
    for parcel in parcels:
        parcel[...] = out[start : start + parcel.shape[0], :]
        start += parcel.shape[0]
    last, first = fields[fields.shape[0] - 1], fields[0]
    edges[0][...] = jnp.where(even, last, first)
    edges[1][...] = jnp.where(even, first, last)


def clear_tail(rows, used):
    start = used // 16 * 16
    rows[:, start:, :] = jnp.zeros((2, rows.shape[1] - start, rows.shape[2]), rows.dtype)


def slopes(normals, trig, k, lo, hi):
    x = normals[0, k : k + 1, lo:hi]
    y = normals[1, k : k + 1, lo:hi]
    return trig[0] * x + trig[1] * y


WEIGHT, REFRACT, SHIFT, EVEN, RISE, FALL, TABLE = 0, 1, 2, 3, 4, 5, 8


def prep_kernel(
    action,
    near,
    sends_in,
    adjacency_in,
    normals_in,
    weight,
    refract,
    shift,
    trig_in,
    *refs,
    routes,
    columns_of,
    groups_out,
    axes,
    unit,
):
    node, freq, count, groups = axes
    total = len(routes)
    parcels, refs = refs[:groups_out], refs[groups_out:]
    edges, refs = refs[:2], refs[2:]
    picks, fields, index_out, normals, nodal, trig = refs[:6]
    rows, neighbours, sends, adjacency, raw, line, arrived, small = refs[6:]
    bands, angles, local = fields.shape
    slots, width = sends.shape[0], sends.shape[2]
    pairs = [
        (near, neighbours),
        (sends_in, sends),
        (adjacency_in, adjacency),
        (normals_in, raw),
        (weight, nodal.at[pl.ds(WEIGHT, 1)]),
        (refract, nodal.at[pl.ds(REFRACT, 1)]),
        (shift, nodal.at[pl.ds(SHIFT, 1)]),
        (trig_in, line),
    ]
    little = [pltpu.make_async_copy(x, y, small.at[i]) for i, (x, y) in enumerate(pairs)]
    copies = [
        pltpu.make_async_copy(action.at[f], fields.at[f], arrived.at[f]) for f in range(bands)
    ]
    for copy in little[:2] + copies + little[2:]:
        copy.start()
    place, band = lax.axis_index(node), lax.axis_index(freq)
    clear_tail(rows, bands * angles)
    for copy in little[:2]:
        copy.wait()
    near_of = [neighbours[0, s] for s in range(slots)]
    table = []
    for route in routes:
        target = target_of(route, place, count)
        slot = jnp.int32(0)
        for s in range(slots):
            slot = jnp.where(near_of[s] == target, s, slot)
        table.append(sends[slot].astype(jnp.float32))
    height = up_to(total, 8)
    if height > total:
        table.append(jnp.zeros((height - total, width), jnp.float32))
    table = jnp.concatenate(table, axis=0)
    if width % 128:
        spare = jnp.zeros((height, up_to(width, 128) - width), jnp.float32)
        table = jnp.concatenate([table, spare], axis=1)
    columns = table.T.astype(jnp.int32)
    lanes = lax.broadcasted_iota(jnp.int32, (width, local), 1)
    for j in range(total):
        hits = lanes == columns[:width, j : j + 1]
        picks[j * width : (j + 1) * width, :] = jnp.where(hits, 1.0, 0.0).astype(jnp.bfloat16)

    def get(f):
        copies[f].wait()
        return fields[f]

    store_groups(rows, get, bands, angles, unit)
    is_even = jnp.full((1, local), band % 2, jnp.int32) == 0
    emit(rows, picks, is_even, fields, parcels, edges)
    for copy in little[2:]:
        copy.wait()
    entry = adjacency[...]
    index = entry
    for s in range(slots):
        column = jnp.int32(0)
        for r, c in zip(routes, columns_of):
            column = jnp.where(near_of[s] == source_of(r, place, count), c, column)
        inside = (entry >= local + s * width) & (entry < local + (s + 1) * width)
        index = jnp.where(inside, entry + column - s * width, index)
    index_out[...] = index
    used = entry != lax.broadcasted_iota(jnp.int32, entry.shape, 1)
    for i in range(2):
        normals[i] = jnp.where(used, raw[i], 0.0)
        trig[i] = jnp.broadcast_to(line[i], trig.shape[1:])
    moved = nodal[SHIFT : SHIFT + 1]
    has_below = jnp.where(band > 0, 1.0, 0.0)
    has_above = jnp.where(band < groups - 1, 1.0, 0.0)
    nodal[EVEN : EVEN + 1] = jnp.where(is_even, 1.0, 0.0)
    nodal[RISE : RISE + 1] = jnp.maximum(moved, 0.0) * has_below
    nodal[FALL : FALL + 1] = jnp.maximum(-moved, 0.0) * has_above
    nodal[FALL + 1 :] = jnp.zeros((TABLE - FALL - 1, local), jnp.float32)


def stack_parcels(stack, halos, arrivals, width):
    depth = stack.shape[1] // 2
    blocks = [halos[g][row : row + width, :] for g, row in arrivals]
    if depth > len(blocks) * width:
        spare = depth - len(blocks) * width
        blocks.append(jnp.zeros((spare, blocks[0].shape[1]), jnp.float32))
    high, low = split(jnp.concatenate(blocks, axis=0).T)
    stack[:, :depth] = high
    stack[:, depth:] = low


def gathered(acc, rows, stack, index, normals, trig, first, bands, angles, unit, finish):
    local = index.shape[1]
    total = up_to(bands * angles, 8)
    waiting = []
    for lo in range(0, local, TILE):
        hi = min(lo + TILE, local)
        for k in range(index.shape[0]):
            entry = index[k : k + 1, lo:hi]
            terms = []
            if rows is not None:
                onehot = hot(entry, 0, local)
                terms += [dot(rows[i, :total, :local], onehot) for i in range(2)]
            if stack is not None:
                onehot = hot(entry, first, stack.shape[1] // 2)
                terms.append(dot(stack[:total], jnp.concatenate([onehot, onehot], axis=0)))
            values = functools.reduce(jnp.add, terms)
            weight = jnp.maximum(-slopes(normals, trig, k, lo, hi), 0.0)
            for g in range(0, bands, unit):
                height = up_to(min(unit, bands - g) * angles, 8)
                window = slice(g * angles, g * angles + height)
                piece = weight[:height] * values[window]
                if k:
                    piece = piece + acc[window, lo:hi]
                acc[window, lo:hi] = piece
            for _ in range(-(-bands // index.shape[0])):
                if waiting:
                    finish(*waiting.pop(0))
        for item in waiting:
            finish(*item)
        waiting = [(f, lo, hi) for f in range(bands)]
    for item in waiting:
        finish(*item)


def local_kernel(*refs, first, arrivals, groups, width, unit):
    halos, refs = refs[:groups], refs[groups:]
    stack = None
    if arrivals:
        stack, refs = refs[-1], refs[:-1]
    if first:
        (action, source_hbm, speeds_hbm, index, normals, nodal, trig) = refs[:7]
        part, invd, invs, base, rows, acc, source, speeds, arrived, came = refs[7:]
        copy = pltpu.make_async_copy(source_hbm, source, arrived)
        copy.start()
        fetch = pltpu.make_async_copy(speeds_hbm, speeds, came)
        fetch.start()
    else:
        (action, invd, invs, base, index, normals, nodal, trig) = refs[:8]
        part, rows, acc = refs[8:]
    bands, angles, local = action.shape
    store_groups(rows, lambda f: action[f], bands, angles, unit)
    if arrivals:
        stack_parcels(stack, halos, arrivals, width)

    def finish(f, lo, hi):
        if first and (f, lo) == (0, 0):
            copy.wait()
            fetch.wait()
        here = action[f, :, lo:hi]
        shift = nodal[SHIFT : SHIFT + 1, lo:hi]
        turning = nodal[REFRACT : REFRACT + 1, lo:hi] * trig[0, :angles, : hi - lo]
        if first:
            outflow = jnp.zeros((angles, hi - lo), jnp.float32)
            wave = [trig[i, :angles, : hi - lo] for i in range(2)]
            weight = nodal[WEIGHT : WEIGHT + 1, lo:hi]
            if f == 0:
                for k in range(index.shape[0]):
                    outflow = outflow + jnp.maximum(slopes(normals, wave, k, lo, hi), 0.0)
                kept[lo] = (outflow, weight + jnp.abs(turning) + jnp.abs(shift))
            outflow, fixed = kept[lo]
            inv = 1.0 / (fixed + speeds[0, f] * outflow)
            start = (weight * here + source[f, :, lo:hi]) * inv
            scaled = speeds[0, f] * inv
            invd[f, :, lo:hi] = inv
            invs[f, :, lo:hi] = scaled
            base[f, :, lo:hi] = start
        else:
            inv, scaled, start = invd[f, :, lo:hi], invs[f, :, lo:hi], base[f, :, lo:hi]
        before = jnp.concatenate([here[angles - 1 :], here[: angles - 1]], axis=0)
        after = jnp.concatenate([here[1:], here[:1]], axis=0)
        inflow = jnp.maximum(turning, 0.0) * before + jnp.maximum(-turning, 0.0) * after
        if f > 0:
            inflow = inflow + jnp.maximum(shift, 0.0) * action[f - 1, :, lo:hi]
        if f < bands - 1:
            inflow = inflow + jnp.maximum(-shift, 0.0) * action[f + 1, :, lo:hi]
        edges = acc[f * angles : (f + 1) * angles, lo:hi]
        part[f, :, lo:hi] = start + inflow * inv + edges * scaled

    kept = {}
    gathered(acc, rows, stack, index, normals, trig, local, bands, angles, unit, finish)


def halo_kernel(*refs, groups, arrivals, first, width, last, unit):
    halos, refs = refs[:groups], refs[groups:]
    (edge_a, edge_b, part, invd, invs, index, normals, nodal, trig), refs = refs[:9], refs[9:]
    if last:
        out, acc, stack = refs
    else:
        picks, out = refs[:2]
        parcels, edges, (acc, stack, rows) = refs[2:-5], refs[-5:-3], refs[-3:]
    bands, angles, _ = part.shape
    stack_parcels(stack, halos, arrivals, width)
    is_even = nodal[EVEN : EVEN + 1, :] > 0.5

    def finish(f, lo, hi):
        value = part[f, :, lo:hi] + acc[f * angles : (f + 1) * angles, lo:hi] * invs[f, :, lo:hi]
        even = is_even[:, lo:hi]
        if f == 0:
            below = jnp.where(even, edge_b[:, lo:hi], edge_a[:, lo:hi])
            value = value + nodal[RISE : RISE + 1, lo:hi] * below * invd[f, :, lo:hi]
        if f == bands - 1:
            above = jnp.where(even, edge_a[:, lo:hi], edge_b[:, lo:hi])
            value = value + nodal[FALL : FALL + 1, lo:hi] * above * invd[f, :, lo:hi]
        out[f, :, lo:hi] = value

    gathered(acc, None, stack, index, normals, trig, first, bands, angles, unit, finish)
    if not last:
        clear_tail(rows, bands * angles)
        store_groups(rows, lambda f: out[f], bands, angles, unit)
        emit(rows, picks, is_even, out, parcels, edges)


def body(
    action_old,
    source,
    time_weight,
    group_speed,
    normals,
    refract,
    freq_shift,
    nbr_list,
    send_nodes,
    adjacency,
):
    bands, angles, local = action_old.shape
    slots, width = send_nodes.shape[1:]
    degree = adjacency.shape[0]
    count = lax.axis_size("node")
    groups = lax.axis_size("freq")
    routes = node_routes(count)
    edge_routes = band_routes(groups)
    plan, relay = plan_of(routes)
    total = len(routes)
    arrivals = [(g, place * width) for g, group in enumerate(plan) for place in range(len(group))]
    if relay:
        arrivals[1] = (relay[1], width)
    early = [
        j
        for j in range(total)
        if relay and routes[j] in (("xor", 6), ("xor", 2))
    ]
    late = [j for j in range(total) if j not in early]
    margin = up_to(len(early) * width, 128)
    columns_of = [
        early.index(j) * width if j in early else margin + late.index(j) * width
        for j in range(total)
    ]
    unit = 8 // math.gcd(angles, 8)
    lanes = up_to(bands * angles, 128)

    theta = 2.0 * math.pi * np.arange(angles).astype(np.float32) / angles
    trig = np.stack([np.cos(theta), np.sin(theta)]).astype(np.float32)[:, :, None]
    trig = jnp.asarray(np.concatenate([trig] * unit, axis=1))

    f32, i32, bf16 = jnp.float32, jnp.int32, jnp.bfloat16
    shape = jax.ShapeDtypeStruct
    cube = shape((bands, angles, local), f32)
    outgoing = [shape((width * len(group), lanes), f32) for group in plan]
    outgoing += [shape((angles, local), f32)] * 2
    tables = [
        shape((total * width, local), bf16),
        cube,
        shape((degree, local), i32),
        shape((2, degree, local), f32),
        shape((TABLE, local), f32),
        shape((2, unit * angles, TILE), f32),
    ]
    rows = pltpu.VMEM((2, lanes, local), bf16)

    def stack(members):
        return pltpu.VMEM((lanes, 2 * up_to(len(members) * width, 128)), bf16)

    def places(members):
        used = sorted({arrivals[j][0] for j in members})
        return used, [(used.index(arrivals[j][0]), arrivals[j][1]) for j in members]

    early_groups, early_arrivals = places(early)
    late_groups, late_arrivals = places(late)
    acc = pltpu.VMEM((up_to(bands * angles, 8), local), f32)
    dma = pltpu.SemaphoreType.DMA
    vmem = pl.BlockSpec(memory_space=pltpu.VMEM)
    far = pl.BlockSpec(memory_space=pltpu.HBM)
    params = pltpu.CompilerParams(vmem_limit_bytes=24 * 2**20)

    def call(kernel, arrays, outs, scratch, depth_rows, distant=(), **options):
        flops = 4 * bands * angles * depth_rows * degree * local
        arrays = [
            pltpu.with_memory_space_constraint(x, pltpu.HBM) if i in distant else x
            for i, x in enumerate(arrays)
        ]
        return pl.pallas_call(
            functools.partial(kernel, unit=unit, **options),
            in_specs=[far if i in distant else vmem for i in range(len(arrays))],
            out_specs=[vmem] * len(outs),
            out_shape=outs,
            scratch_shapes=scratch,
            compiler_params=params,
            cost_estimate=pl.CostEstimate(
                flops=flops, transcendentals=0, bytes_accessed=4 * bands * angles * local
            ),
        )(*arrays)

    nodal = [x.reshape(1, local) for x in (time_weight, refract, freq_shift)]
    prepared = call(
        prep_kernel,
        [action_old, nbr_list, send_nodes.reshape(slots, 1, width), adjacency, normals, *nodal, trig],
        outgoing + tables,
        [
            rows,
            pltpu.SMEM((1, slots), i32),
            pltpu.VMEM((slots, 1, width), i32),
            pltpu.VMEM((degree, local), i32),
            pltpu.VMEM((2, degree, local), f32),
            pltpu.VMEM(trig.shape, f32),
            dma((bands,)),
            dma((8,)),
        ],
        0,
        distant=range(9),
        routes=routes,
        columns_of=columns_of,
        groups_out=len(plan),
        axes=("node", "freq", count, groups),
    )
    sends = prepared[: len(outgoing)]
    picks, spectra, *shared = prepared[len(outgoing) :]

    def along(block, group):
        route = routes[plan[group][0]]
        return lax.ppermute(block, "node", [(p, target_of(route, p, count)) for p in range(count)])

    for step in range(ITERS):
        direct = [g for g in range(len(plan)) if not relay or g != relay[1]]
        arrived = {}
        for g in direct:
            arrived[g] = along(sends[g], g)
        across = [
            lax.ppermute(x, "freq", list(enumerate(r)))
            for x, r in zip(sends[len(plan) :], edge_routes)
        ]
        if relay:
            passed = jnp.concatenate([sends[relay[1]], arrived[relay[0]][width:]], axis=0)
            passed, spectra = lax.optimization_barrier((passed, spectra))
            arrived[relay[1]] = along(passed, relay[1])
        ahead = [arrived[g] for g in early_groups]
        after = [arrived[g] for g in late_groups] + across
        window = dict(arrivals=early_arrivals, groups=len(early_groups), width=width)
        stacks = [stack(early)] if early else []
        depth = local + margin // 2
        if step == 0:
            part, invd, invs, base = call(
                local_kernel,
                [*ahead, spectra, source, group_speed.reshape(1, bands), *shared],
                [cube] * 4,
                [
                    rows,
                    acc,
                    pltpu.VMEM((bands, angles, local), f32),
                    pltpu.SMEM((1, bands), f32),
                    dma,
                    dma,
                    *stacks,
                ],
                depth,
                distant=(len(ahead) + 1, len(ahead) + 2),
                first=True,
                **window,
            )
        else:
            (part,) = call(
                local_kernel,
                [*ahead, spectra, invd, invs, base, *shared],
                [cube],
                [rows, acc, *stacks],
                depth,
                first=False,
                **window,
            )
        last = step == ITERS - 1
        spectra, *sends = call(
            halo_kernel,
            [*after, part, invd, invs, *shared] + ([] if last else [picks]),
            [cube] + ([] if last else outgoing),
            [acc, stack(late)] + ([] if last else [rows]),
            up_to(len(late) * width, 128),
            groups=len(late_groups),
            arrivals=late_arrivals,
            first=local + margin,
            width=width,
            last=last,
        )
    return spectra


def solution(mesh):
    in_specs = (
        P("freq", None, "node"),
        P("freq", None, "node"),
        P("node"),
        P("freq"),
        P(None, None, "node"),
        P("node"),
        P("node"),
        P("node", None),
        P("node", None, None),
        P(None, "node"),
    )
    out_specs = P("freq", None, "node")
    return jax.shard_map(body, mesh=mesh, in_specs=in_specs, out_specs=out_specs, check_vma=False)
```

```python
import functools
import math

import jax
import jax.numpy as jnp
import numpy as np
from jax import lax
from jax.experimental import pallas as pl
from jax.experimental.pallas import tpu as pltpu
from jax.sharding import PartitionSpec as P


REACH = 3
ITERS = 3
TILE = 256


def up_to(value, multiple):
    return -(-value // multiple) * multiple


def node_routes(count):
    masks = {p ^ ((p + d) % count) for p in range(count) for d in range(1, REACH + 1)}
    if count & (count - 1) == 0 and len(masks) <= 2 * REACH:
        order = [m for m in (6, 7, 2, 3, 5, 1) if m in masks]
        return [("xor", m) for m in order + sorted(masks - set(order))]
    routes = []
    for d in range(REACH, 0, -1):
        step = d & -d
        if count % (2 * step) == 0 and count > 2 * d:
            routes += [("swap", d, step, 0), ("swap", d, step, 1)]
        else:
            routes += [("shift", d), ("shift", -d)]
    return routes


def target_of(route, place, count):
    if route[0] == "xor":
        return place ^ route[1]
    if route[0] == "shift":
        return (place + route[1] + count) % count
    _, d, step, side = route
    turn = 1 - 2 * (((place // step) % 2) ^ side)
    return (place + turn * d + count) % count


def source_of(route, place, count):
    if route[0] == "shift":
        return target_of(("shift", -route[1]), place, count)
    return target_of(route, place, count)


def plan_of(routes):
    if routes[:2] == [("xor", 6), ("xor", 7)] and routes[-1] == ("xor", 1):
        groups = [[0, 1]] + [[j] for j in range(2, len(routes))]
        return groups, (0, len(groups) - 1)
    return [[j] for j in range(len(routes))], None


def band_routes(count):
    first = [(p ^ 1) if (p ^ 1) < count else p for p in range(count)]
    second = [p if p == 0 else p + (1 if p % 2 else -1) for p in range(count)]
    second = [q if q < count else p for p, q in enumerate(second)]
    if count % 2 == 0:
        second[0], second[-1] = count - 1, 0
    return [first, second]


def split(values):
    high = values.astype(jnp.bfloat16)
    low = (values - high.astype(jnp.float32)).astype(jnp.bfloat16)
    return high, low


def hot(index, first, rows):
    step = min(rows, 256)
    shape = (step, index.shape[1])
    ids = lax.broadcasted_iota(jnp.int32, shape, 0).astype(jnp.float32).astype(jnp.bfloat16)
    blocks = []
    for start in range(0, rows, step):
        offset = (index - (first + start)).astype(jnp.float32).astype(jnp.bfloat16)
        hits = ids == jnp.broadcast_to(offset, shape)
        blocks.append(jnp.where(hits, jnp.bfloat16(1), jnp.bfloat16(0)))
    return blocks[0] if len(blocks) == 1 else jnp.concatenate(blocks, axis=0)


def dot(left, right, contract=((1,), (0,))):
    return lax.dot_general(left, right, (contract, ((), ())), preferred_element_type=jnp.float32)


def store_groups(rows, get, bands, angles, unit):
    for g in range(0, bands, unit):
        values = [get(f) for f in range(g, min(g + unit, bands))]
        block = values[0] if len(values) == 1 else jnp.concatenate(values, axis=0)
        tail = up_to(block.shape[0], 8) - block.shape[0]
        if tail:
            block = jnp.concatenate([block, jnp.zeros((tail, block.shape[1]), jnp.float32)], axis=0)
        high, low = split(block)
        window = slice(g * angles, g * angles + block.shape[0])
        rows[0, window, : block.shape[1]] = high
        rows[1, window, : block.shape[1]] = low


def emit(rows, picks, even, fields, parcels, edges):
    local = fields.shape[2]
    nt = ((1,), (1,))
    chosen = picks[...]
    out = dot(chosen, rows[0, :, :local], nt) + dot(chosen, rows[1, :, :local], nt)
    start = 0
    for parcel in parcels:
        parcel[...] = out[start : start + parcel.shape[0], :]
        start += parcel.shape[0]
    last, first = fields[fields.shape[0] - 1], fields[0]
    edges[0][...] = jnp.where(even, last, first)
    edges[1][...] = jnp.where(even, first, last)


def clear_tail(rows, used):
    start = used // 16 * 16
    rows[:, start:, :] = jnp.zeros((2, rows.shape[1] - start, rows.shape[2]), rows.dtype)


def slopes(normals, trig, k, lo, hi):
    x = normals[0, k : k + 1, lo:hi]
    y = normals[1, k : k + 1, lo:hi]
    return trig[0] * x + trig[1] * y


WEIGHT, REFRACT, SHIFT, EVEN, RISE, FALL, TABLE = 0, 1, 2, 3, 4, 5, 8


def prep_kernel(
    action,
    near,
    sends_in,
    adjacency_in,
    normals_in,
    weight,
    refract,
    shift,
    trig_in,
    *refs,
    routes,
    columns_of,
    groups_out,
    axes,
    unit,
):
    node, freq, count, groups = axes
    total = len(routes)
    parcels, refs = refs[:groups_out], refs[groups_out:]
    edges, refs = refs[:2], refs[2:]
    picks, fields, index_out, normals, nodal, trig = refs[:6]
    rows, neighbours, sends, adjacency, raw, line, arrived, small = refs[6:]
    bands, angles, local = fields.shape
    slots, width = sends.shape[0], sends.shape[2]
    pairs = [
        (near, neighbours),
        (sends_in, sends),
        (adjacency_in, adjacency),
        (normals_in, raw),
        (weight, nodal.at[pl.ds(WEIGHT, 1)]),
        (refract, nodal.at[pl.ds(REFRACT, 1)]),
        (shift, nodal.at[pl.ds(SHIFT, 1)]),
        (trig_in, line),
    ]
    little = [pltpu.make_async_copy(x, y, small.at[i]) for i, (x, y) in enumerate(pairs)]
    copies = [
        pltpu.make_async_copy(action.at[f], fields.at[f], arrived.at[f]) for f in range(bands)
    ]
    for copy in little[:2] + copies + little[2:]:
        copy.start()
    place, band = lax.axis_index(node), lax.axis_index(freq)
    clear_tail(rows, bands * angles)
    for copy in little[:2]:
        copy.wait()
    near_of = [neighbours[0, s] for s in range(slots)]
    table = []
    for route in routes:
        target = target_of(route, place, count)
        slot = jnp.int32(0)
        for s in range(slots):
            slot = jnp.where(near_of[s] == target, s, slot)
        table.append(sends[slot].astype(jnp.float32))
    height = up_to(total, 8)
    if height > total:
        table.append(jnp.zeros((height - total, width), jnp.float32))
    table = jnp.concatenate(table, axis=0)
    if width % 128:
        spare = jnp.zeros((height, up_to(width, 128) - width), jnp.float32)
        table = jnp.concatenate([table, spare], axis=1)
    columns = table.T.astype(jnp.int32)
    lanes = lax.broadcasted_iota(jnp.int32, (width, local), 1)
    for j in range(total):
        hits = lanes == columns[:width, j : j + 1]
        picks[j * width : (j + 1) * width, :] = jnp.where(hits, 1.0, 0.0).astype(jnp.bfloat16)

    def get(f):
        copies[f].wait()
        return fields[f]

    store_groups(rows, get, bands, angles, unit)
    is_even = jnp.full((1, local), band % 2, jnp.int32) == 0
    emit(rows, picks, is_even, fields, parcels, edges)
    for copy in little[2:]:
        copy.wait()
    entry = adjacency[...]
    index = entry
    for s in range(slots):
        column = jnp.int32(0)
        for r, c in zip(routes, columns_of):
            column = jnp.where(near_of[s] == source_of(r, place, count), c, column)
        inside = (entry >= local + s * width) & (entry < local + (s + 1) * width)
        index = jnp.where(inside, entry + column - s * width, index)
    index_out[...] = index
    used = entry != lax.broadcasted_iota(jnp.int32, entry.shape, 1)
    for i in range(2):
        normals[i] = jnp.where(used, raw[i], 0.0)
        trig[i] = jnp.broadcast_to(line[i], trig.shape[1:])
    moved = nodal[SHIFT : SHIFT + 1]
    has_below = jnp.where(band > 0, 1.0, 0.0)
    has_above = jnp.where(band < groups - 1, 1.0, 0.0)
    nodal[EVEN : EVEN + 1] = jnp.where(is_even, 1.0, 0.0)
    nodal[RISE : RISE + 1] = jnp.maximum(moved, 0.0) * has_below
    nodal[FALL : FALL + 1] = jnp.maximum(-moved, 0.0) * has_above
    nodal[FALL + 1 :] = jnp.zeros((TABLE - FALL - 1, local), jnp.float32)


def stack_parcels(stack, halos, arrivals, width):
    depth = stack.shape[1] // 2
    blocks = [halos[g][row : row + width, :] for g, row in arrivals]
    if depth > len(blocks) * width:
        spare = depth - len(blocks) * width
        blocks.append(jnp.zeros((spare, blocks[0].shape[1]), jnp.float32))
    high, low = split(jnp.concatenate(blocks, axis=0).T)
    stack[:, :depth] = high
    stack[:, depth:] = low


def gathered(acc, rows, stack, index, normals, trig, first, bands, angles, unit, finish):
    local = index.shape[1]
    total = up_to(bands * angles, 8)
    waiting = []
    for lo in range(0, local, TILE):
        hi = min(lo + TILE, local)
        for k in range(index.shape[0]):
            entry = index[k : k + 1, lo:hi]
            terms = []
            if rows is not None:
                onehot = hot(entry, 0, local)
                terms += [dot(rows[i, :total, :local], onehot) for i in range(2)]
            if stack is not None:
                onehot = hot(entry, first, stack.shape[1] // 2)
                terms.append(dot(stack[:total], jnp.concatenate([onehot, onehot], axis=0)))
            values = functools.reduce(jnp.add, terms)
            weight = jnp.maximum(-slopes(normals, trig, k, lo, hi), 0.0)
            for g in range(0, bands, unit):
                height = up_to(min(unit, bands - g) * angles, 8)
                window = slice(g * angles, g * angles + height)
                piece = weight[:height] * values[window]
                if k:
                    piece = piece + acc[window, lo:hi]
                acc[window, lo:hi] = piece
            for _ in range(-(-bands // index.shape[0])):
                if waiting:
                    finish(*waiting.pop(0))
        for item in waiting:
            finish(*item)
        waiting = [(f, lo, hi) for f in range(bands)]
    for item in waiting:
        finish(*item)


def local_kernel(*refs, first, arrivals, groups, width, unit):
    halos, refs = refs[:groups], refs[groups:]
    stack = None
    if arrivals:
        stack, refs = refs[-1], refs[:-1]
    if first:
        (action, source_hbm, speeds_hbm, index, normals, nodal, trig) = refs[:7]
        part, invd, invs, base, rows, acc, source, speeds, arrived, came = refs[7:]
        copy = pltpu.make_async_copy(source_hbm, source, arrived)
        copy.start()
        fetch = pltpu.make_async_copy(speeds_hbm, speeds, came)
        fetch.start()
    else:
        (action, invd, invs, base, index, normals, nodal, trig) = refs[:8]
        part, rows, acc = refs[8:]
    bands, angles, local = action.shape
    store_groups(rows, lambda f: action[f], bands, angles, unit)
    if arrivals:
        stack_parcels(stack, halos, arrivals, width)

    def finish(f, lo, hi):
        if first and (f, lo) == (0, 0):
            copy.wait()
            fetch.wait()
        here = action[f, :, lo:hi]
        shift = nodal[SHIFT : SHIFT + 1, lo:hi]
        turning = nodal[REFRACT : REFRACT + 1, lo:hi] * trig[0, :angles, : hi - lo]
        if first:
            outflow = jnp.zeros((angles, hi - lo), jnp.float32)
            wave = [trig[i, :angles, : hi - lo] for i in range(2)]
            weight = nodal[WEIGHT : WEIGHT + 1, lo:hi]
            if f == 0:
                for k in range(index.shape[0]):
                    outflow = outflow + jnp.maximum(slopes(normals, wave, k, lo, hi), 0.0)
                kept[lo] = (outflow, weight + jnp.abs(turning) + jnp.abs(shift))
            outflow, fixed = kept[lo]
            inv = 1.0 / (fixed + speeds[0, f] * outflow)
            start = (weight * here + source[f, :, lo:hi]) * inv
            scaled = speeds[0, f] * inv
            invd[f, :, lo:hi] = inv
            invs[f, :, lo:hi] = scaled
            base[f, :, lo:hi] = start
        else:
            inv, scaled, start = invd[f, :, lo:hi], invs[f, :, lo:hi], base[f, :, lo:hi]
        before = jnp.concatenate([here[angles - 1 :], here[: angles - 1]], axis=0)
        after = jnp.concatenate([here[1:], here[:1]], axis=0)
        inflow = jnp.maximum(turning, 0.0) * before + jnp.maximum(-turning, 0.0) * after
        if f > 0:
            inflow = inflow + jnp.maximum(shift, 0.0) * action[f - 1, :, lo:hi]
        if f < bands - 1:
            inflow = inflow + jnp.maximum(-shift, 0.0) * action[f + 1, :, lo:hi]
        edges = acc[f * angles : (f + 1) * angles, lo:hi]
        part[f, :, lo:hi] = start + inflow * inv + edges * scaled

    kept = {}
    gathered(acc, rows, stack, index, normals, trig, local, bands, angles, unit, finish)


def halo_kernel(*refs, groups, arrivals, first, width, last, unit):
    halos, refs = refs[:groups], refs[groups:]
    (edge_a, edge_b, part, invd, invs, index, normals, nodal, trig), refs = refs[:9], refs[9:]
    if last:
        out, acc, stack = refs
    else:
        picks, out = refs[:2]
        parcels, edges, (acc, stack, rows) = refs[2:-5], refs[-5:-3], refs[-3:]
    bands, angles, _ = part.shape
    stack_parcels(stack, halos, arrivals, width)
    is_even = nodal[EVEN : EVEN + 1, :] > 0.5

    def finish(f, lo, hi):
        value = part[f, :, lo:hi] + acc[f * angles : (f + 1) * angles, lo:hi] * invs[f, :, lo:hi]
        even = is_even[:, lo:hi]
        if f == 0:
            below = jnp.where(even, edge_b[:, lo:hi], edge_a[:, lo:hi])
            value = value + nodal[RISE : RISE + 1, lo:hi] * below * invd[f, :, lo:hi]
        if f == bands - 1:
            above = jnp.where(even, edge_a[:, lo:hi], edge_b[:, lo:hi])
            value = value + nodal[FALL : FALL + 1, lo:hi] * above * invd[f, :, lo:hi]
        out[f, :, lo:hi] = value

    gathered(acc, None, stack, index, normals, trig, first, bands, angles, unit, finish)
    if not last:
        clear_tail(rows, bands * angles)
        store_groups(rows, lambda f: out[f], bands, angles, unit)
        emit(rows, picks, is_even, out, parcels, edges)


def body(
    action_old,
    source,
    time_weight,
    group_speed,
    normals,
    refract,
    freq_shift,
    nbr_list,
    send_nodes,
    adjacency,
):
    bands, angles, local = action_old.shape
    slots, width = send_nodes.shape[1:]
    degree = adjacency.shape[0]
    count = lax.axis_size("node")
    groups = lax.axis_size("freq")
    routes = node_routes(count)
    edge_routes = band_routes(groups)
    plan, relay = plan_of(routes)
    total = len(routes)
    arrivals = [(g, place * width) for g, group in enumerate(plan) for place in range(len(group))]
    if relay:
        arrivals[1] = (relay[1], width)
    early = [
        j
        for j in range(total)
        if relay and routes[j] in (("xor", 6), ("xor", 2))
    ]
    late = [j for j in range(total) if j not in early]
    margin = up_to(len(early) * width, 128)
    columns_of = [
        early.index(j) * width if j in early else margin + late.index(j) * width
        for j in range(total)
    ]
    unit = 8 // math.gcd(angles, 8)
    lanes = up_to(bands * angles, 128)

    theta = 2.0 * math.pi * np.arange(angles).astype(np.float32) / angles
    trig = np.stack([np.cos(theta), np.sin(theta)]).astype(np.float32)[:, :, None]
    trig = jnp.asarray(np.concatenate([trig] * unit, axis=1))

    f32, i32, bf16 = jnp.float32, jnp.int32, jnp.bfloat16
    shape = jax.ShapeDtypeStruct
    cube = shape((bands, angles, local), f32)
    outgoing = [shape((width * len(group), lanes), f32) for group in plan]
    outgoing += [shape((angles, local), f32)] * 2
    tables = [
        shape((total * width, local), bf16),
        cube,
        shape((degree, local), i32),
        shape((2, degree, local), f32),
        shape((TABLE, local), f32),
        shape((2, unit * angles, TILE), f32),
    ]
    rows = pltpu.VMEM((2, lanes, local), bf16)

    def stack(members):
        return pltpu.VMEM((lanes, 2 * up_to(len(members) * width, 128)), bf16)

    def places(members):
        used = sorted({arrivals[j][0] for j in members})
        return used, [(used.index(arrivals[j][0]), arrivals[j][1]) for j in members]

    early_groups, early_arrivals = places(early)
    late_groups, late_arrivals = places(late)
    acc = pltpu.VMEM((up_to(bands * angles, 8), local), f32)
    dma = pltpu.SemaphoreType.DMA
    vmem = pl.BlockSpec(memory_space=pltpu.VMEM)
    far = pl.BlockSpec(memory_space=pltpu.HBM)
    params = pltpu.CompilerParams(vmem_limit_bytes=24 * 2**20)

    def call(kernel, arrays, outs, scratch, depth_rows, distant=(), **options):
        flops = 4 * bands * angles * depth_rows * degree * local
        arrays = [
            pltpu.with_memory_space_constraint(x, pltpu.HBM) if i in distant else x
            for i, x in enumerate(arrays)
        ]
        return pl.pallas_call(
            functools.partial(kernel, unit=unit, **options),
            in_specs=[far if i in distant else vmem for i in range(len(arrays))],
            out_specs=[vmem] * len(outs),
            out_shape=outs,
            scratch_shapes=scratch,
            compiler_params=params,
            cost_estimate=pl.CostEstimate(
                flops=flops, transcendentals=0, bytes_accessed=4 * bands * angles * local
            ),
        )(*arrays)

    nodal = [x.reshape(1, local) for x in (time_weight, refract, freq_shift)]
    prepared = call(
        prep_kernel,
        [action_old, nbr_list, send_nodes.reshape(slots, 1, width), adjacency, normals, *nodal, trig],
        outgoing + tables,
        [
            rows,
            pltpu.SMEM((1, slots), i32),
            pltpu.VMEM((slots, 1, width), i32),
            pltpu.VMEM((degree, local), i32),
            pltpu.VMEM((2, degree, local), f32),
            pltpu.VMEM(trig.shape, f32),
            dma((bands,)),
            dma((8,)),
        ],
        0,
        distant=range(9),
        routes=routes,
        columns_of=columns_of,
        groups_out=len(plan),
        axes=("node", "freq", count, groups),
    )
    sends = prepared[: len(outgoing)]
    picks, spectra, *shared = prepared[len(outgoing) :]

    def along(block, group):
        route = routes[plan[group][0]]
        return lax.ppermute(block, "node", [(p, target_of(route, p, count)) for p in range(count)])

    for step in range(ITERS):
        direct = [g for g in range(len(plan)) if not relay or g != relay[1]]
        arrived = {}
        for g in direct:
            arrived[g] = along(sends[g], g)
        across = []
        for x, r in zip(sends[len(plan) :], edge_routes):
            across.append(lax.ppermute(x, "freq", list(enumerate(r))))
        if relay:
            passed = jnp.concatenate([sends[relay[1]], arrived[relay[0]][width:]], axis=0)
            passed, spectra = lax.optimization_barrier((passed, spectra))
            arrived[relay[1]] = along(passed, relay[1])
        ahead = [arrived[g] for g in early_groups]
        after = [arrived[g] for g in late_groups] + across
        window = dict(arrivals=early_arrivals, groups=len(early_groups), width=width)
        stacks = [stack(early)] if early else []
        depth = local + margin // 2
        if step == 0:
            part, invd, invs, base = call(
                local_kernel,
                [*ahead, spectra, source, group_speed.reshape(1, bands), *shared],
                [cube] * 4,
                [
                    rows,
                    acc,
                    pltpu.VMEM((bands, angles, local), f32),
                    pltpu.SMEM((1, bands), f32),
                    dma,
                    dma,
                    *stacks,
                ],
                depth,
                distant=(len(ahead) + 1, len(ahead) + 2),
                first=True,
                **window,
            )
        else:
            (part,) = call(
                local_kernel,
                [*ahead, spectra, invd, invs, base, *shared],
                [cube],
                [rows, acc, *stacks],
                depth,
                first=False,
                **window,
            )
        last = step == ITERS - 1
        spectra, *sends = call(
            halo_kernel,
            [*after, part, invd, invs, *shared] + ([] if last else [picks]),
            [cube] + ([] if last else outgoing),
            [acc, stack(late)] + ([] if last else [rows]),
            up_to(len(late) * width, 128),
            groups=len(late_groups),
            arrivals=late_arrivals,
            first=local + margin,
            width=width,
            last=last,
        )
    return spectra


def solution(mesh):
    in_specs = (
        P("freq", None, "node"),
        P("freq", None, "node"),
        P("node"),
        P("freq"),
        P(None, None, "node"),
        P("node"),
        P("node"),
        P("node", None),
        P("node", None, None),
        P(None, "node"),
    )
    out_specs = P("freq", None, "node")
    return jax.shard_map(body, mesh=mesh, in_specs=in_specs, out_specs=out_specs, check_vma=False)
```
